8 devices in a mesh: node: 2 (over z, y), local: 4 (over x, core).
Axes of the slice: x: 2, y: 2, z: 1, core: 2. Of those that a mesh axis runs over, the one named last changes fastest.
Arguments:
- x: bfloat16 [48, 128, 768], P(('node', 'local'))
- y_cot: bfloat16 [48, 128, 768], P(('node', 'local'))
- ln1_gain: bfloat16 [2, 768], P(None, ('node', 'local'))
- ln1_bias: bfloat16 [2, 768], P(None, ('node', 'local'))
- qkv_weight: bfloat16 [2, 768, 12, 192], P(None, ('node', 'local'))
- qkv_bias: bfloat16 [2, 2304], P(None, ('node', 'local'))
- out_weight: bfloat16 [2, 768, 768], P(None, ('node', 'local'))
- out_bias: bfloat16 [2, 768], P(None, ('node', 'local'))
- ln2_gain: bfloat16 [2, 768], P(None, ('node', 'local'))
- ln2_bias: bfloat16 [2, 768], P(None, ('node', 'local'))
- up_weight: bfloat16 [2, 768, 3072], P(None, ('node', 'local'))
- up_bias: bfloat16 [2, 3072], P(None, ('node', 'local'))
- down_weight: bfloat16 [2, 3072, 768], P(None, ('node', 'local'))
- down_bias: bfloat16 [2, 768], P(None, ('node', 'local'))
Outputs:
- output 1: bfloat16 [48, 128, 768], P(('node', 'local'))
- output 2: bfloat16 [48, 128, 768], P(('node', 'local'))
- output 3: bfloat16 [2, 768], P(None, ('node', 'local'))
- output 4: bfloat16 [2, 768], P(None, ('node', 'local'))
- output 5: bfloat16 [2, 768, 12, 192], P(None, ('node', 'local'))
- output 6: bfloat16 [2, 2304], P(None, ('node', 'local'))
- output 7: bfloat16 [2, 768, 768], P(None, ('node', 'local'))
- output 8: bfloat16 [2, 768], P(None, ('node', 'local'))
- output 9: bfloat16 [2, 768], P(None, ('node', 'local'))
- output 10: bfloat16 [2, 768], P(None, ('node', 'local'))
- output 11: bfloat16 [2, 768, 3072], P(None, ('node', 'local'))
- output 12: bfloat16 [2, 3072], P(None, ('node', 'local'))
- output 13: bfloat16 [2, 3072, 768], P(None, ('node', 'local'))
- output 14: bfloat16 [2, 768], P(None, ('node', 'local'))
All inputs are finite; a program needn't handle non-finite values.
Results may differ from the reference program's by a relative error of at most 0.0160448.
Values are sent between devices in bfloat16 or wider.
A program may use at most 1 GiB of HBM per device.

```python
import jax
import jax.numpy as jnp
from jax import lax

D_MODEL = 768
HEADS = 12
SEQ_LEN = 128
BATCH = 48
LAYERS = 2
HEAD_DIM = D_MODEL // HEADS
ROT_DIM = HEAD_DIM // 4
FF_DIM = 4 * D_MODEL
EPSILON = 1e-5


def slow_waves(rng_key, frequencies):
    amp_key, phase_key = jax.random.split(rng_key)
    positions = jnp.arange(SEQ_LEN, dtype=jnp.float32)[None, :, None] / SEQ_LEN
    wave_sum = jnp.zeros((BATCH, SEQ_LEN, D_MODEL), jnp.float32)
    for wave_idx, frequency in enumerate(frequencies):
        amplitude = jax.random.normal(jax.random.fold_in(amp_key, wave_idx), (BATCH, 1, D_MODEL), jnp.float32)
        phase_off = jax.random.uniform(jax.random.fold_in(phase_key, wave_idx), (BATCH, 1, D_MODEL), jnp.float32, 0.0, 6.283185307179586)
        wave_sum = wave_sum + amplitude * jnp.cos(6.283185307179586 * frequency * positions + phase_off)
    return wave_sum * (2.0 / len(frequencies)) ** 0.5


def normal_draw(rng_key, out_shape, spread, offset=0.0):
    return (offset + spread * jax.random.normal(rng_key, out_shape, jnp.float32)).astype(jnp.bfloat16)


def setup_inputs(seed: int = 0) -> dict:
    sub_keys = jax.random.split(jax.random.key(seed), 16)
    white_noise = jax.random.normal(sub_keys[0], (BATCH, SEQ_LEN, D_MODEL), jnp.float32)
    x = (0.8 * slow_waves(sub_keys[1], (0.5, 1.0, 2.0, 3.0)) + 0.6 * white_noise).astype(jnp.bfloat16)
    y_cot = normal_draw(sub_keys[2], (BATCH, SEQ_LEN, D_MODEL), (BATCH * SEQ_LEN) ** -0.25)
    width_scale = D_MODEL ** -0.5
    return {
        'x': x,
        'y_cot': y_cot,
        'ln1_gain': normal_draw(sub_keys[3], (LAYERS, D_MODEL), 0.25, 1.0),
        'ln1_bias': normal_draw(sub_keys[4], (LAYERS, D_MODEL), 0.25),
        'qkv_weight': normal_draw(sub_keys[5], (LAYERS, D_MODEL, HEADS, 3 * HEAD_DIM), width_scale),
        'qkv_bias': normal_draw(sub_keys[6], (LAYERS, 3 * D_MODEL), 0.3),
        'out_weight': normal_draw(sub_keys[7], (LAYERS, D_MODEL, D_MODEL), 1.5 * width_scale),
        'out_bias': normal_draw(sub_keys[8], (LAYERS, D_MODEL), 0.3),
        'ln2_gain': normal_draw(sub_keys[9], (LAYERS, D_MODEL), 0.25, 1.0),
        'ln2_bias': normal_draw(sub_keys[10], (LAYERS, D_MODEL), 0.25),
        'up_weight': normal_draw(sub_keys[11], (LAYERS, D_MODEL, FF_DIM), width_scale),
        'up_bias': normal_draw(sub_keys[12], (LAYERS, FF_DIM), 0.3),
        'down_weight': normal_draw(sub_keys[13], (LAYERS, FF_DIM, D_MODEL), FF_DIM ** -0.5),
        'down_bias': normal_draw(sub_keys[14], (LAYERS, D_MODEL), 0.3),
    }


def to_bf16(values):
    return values.astype(jnp.bfloat16).astype(jnp.float32)


def rope_tables():
    inv_freq = 1.0 / (10000.0 ** (jnp.arange(0, ROT_DIM, 2, dtype=jnp.float32) / ROT_DIM))
    angles = jnp.arange(SEQ_LEN, dtype=jnp.float32)[:, None] * inv_freq[None, :]
    angles = jnp.concatenate([angles, angles], axis=-1)
    return jnp.cos(angles), jnp.sin(angles)


def apply_rotary(vectors, cos_tab, sin_tab):
    half_dim = ROT_DIM // 2
    rot_part = vectors[..., :ROT_DIM]
    pass_part = vectors[..., ROT_DIM:]
    turned = jnp.concatenate([-rot_part[..., half_dim:], rot_part[..., :half_dim]], axis=-1)
    rot_part = rot_part * cos_tab[:, None, :] + turned * sin_tab[:, None, :]
    return jnp.concatenate([rot_part, pass_part], axis=-1)


def layer_norm(hidden, ln_gain, ln_bias):
    center = hidden - jnp.mean(hidden, axis=-1, keepdims=True)
    variance = jnp.mean(center * center, axis=-1, keepdims=True)
    return center * lax.rsqrt(variance + EPSILON) * ln_gain + ln_bias


def layer_forward(hidden, weights, cos_tab, sin_tab):
    (ln1_gain, ln1_bias, qkv_weight, qkv_bias, out_weight, out_bias,
     ln2_gain, ln2_bias, up_weight, up_bias, down_weight, down_bias) = weights
    normed_attn = to_bf16(layer_norm(hidden, ln1_gain, ln1_bias))
    normed_mlp = to_bf16(layer_norm(hidden, ln2_gain, ln2_bias))
    qkv_all = jnp.einsum('sd,dhe->she', normed_attn, qkv_weight) + qkv_bias.reshape(HEADS, 3 * HEAD_DIM)
    query_rot = to_bf16(apply_rotary(qkv_all[..., :HEAD_DIM], cos_tab, sin_tab))
    key_rot = to_bf16(apply_rotary(qkv_all[..., HEAD_DIM:2 * HEAD_DIM], cos_tab, sin_tab))
    values = to_bf16(qkv_all[..., 2 * HEAD_DIM:])
    scores = jnp.einsum('qhd,khd->hqk', query_rot, key_rot) * HEAD_DIM ** -0.5
    causal = jnp.arange(SEQ_LEN)[:, None] >= jnp.arange(SEQ_LEN)[None, :]
    scores = jnp.where(causal[None], scores, -1e30)
    attn_probs = to_bf16(jax.nn.softmax(scores, axis=-1))
    context = to_bf16(jnp.einsum('hqk,khd->qhd', attn_probs, values))
    attn_out = jnp.einsum('qhd,hde->qe', context, out_weight.reshape(HEADS, HEAD_DIM, D_MODEL)) + out_bias
    mlp_act = to_bf16(jax.nn.gelu(jnp.dot(normed_mlp, up_weight) + up_bias, approximate=False))
    mlp_out = jnp.dot(mlp_act, down_weight) + down_bias
    return hidden + attn_out + mlp_out


def reference(x, y_cot, ln1_gain, ln1_bias, qkv_weight, qkv_bias, out_weight, out_bias,
              ln2_gain, ln2_bias, up_weight, up_bias, down_weight, down_bias):
    stacked = tuple(tensor.astype(jnp.float32) for tensor in (
        ln1_gain, ln1_bias, qkv_weight, qkv_bias, out_weight, out_bias,
        ln2_gain, ln2_bias, up_weight, up_bias, down_weight, down_bias))
    cos_tab, sin_tab = rope_tables()

    def both_layers(x_seq, params):
        hidden = x_seq
        for layer_idx in range(LAYERS):
            hidden = to_bf16(layer_forward(hidden, [tensor[layer_idx] for tensor in params], cos_tab, sin_tab))
        return hidden

    def seq_step(grad_sums, seq_pair):
        x_seq, cot_seq = seq_pair
        seq_out, pullback = jax.vjp(both_layers, x_seq.astype(jnp.float32), stacked)
        x_bar, param_bars = pullback(cot_seq.astype(jnp.float32))
        grad_sums = tuple(grad_sum + part_grad for grad_sum, part_grad in zip(grad_sums, param_bars))
        return grad_sums, (seq_out.astype(jnp.bfloat16), x_bar.astype(jnp.bfloat16))

    zero_sums = tuple(jnp.zeros_like(tensor) for tensor in stacked)
    grad_sums, (y_out, x_grad) = lax.scan(seq_step, zero_sums, (x, y_cot))
    grad_list = [grad_sum.astype(jnp.bfloat16) for grad_sum in grad_sums]
    return (y_out, x_grad, grad_list[0], grad_list[1], grad_list[2], grad_list[3], grad_list[4], grad_list[5],
            grad_list[6], grad_list[7], grad_list[8], grad_list[9], grad_list[10], grad_list[11])
```

```python
import functools
import jax
import jax.numpy as jnp
from jax import lax
from jax.experimental import pallas as pl
from jax.experimental.pallas import tpu as pltpu
from jax.sharding import PartitionSpec as P

EPSILON = 1e-5
BF = jnp.bfloat16
F32 = jnp.float32
AXES = ('node', 'local')
SQRT_HALF = 0.7071067811865476
INV_SQRT_2PI = 0.3989422804014327
VMEM = pl.BlockSpec(memory_space=pltpu.VMEM)
ANY = pl.BlockSpec(memory_space=pl.ANY)


def pairs(move):
    out = []
    for n in range(2):
        for x in range(2):
            for c in range(2):
                n2, x2, c2 = move(n, x, c)
                out.append((n * 4 + x * 2 + c, n2 * 4 + x2 * 2 + c2))
    return out


TO_X = pairs(lambda n, x, c: (n, 1 - x, c))
TO_Y = pairs(lambda n, x, c: (1 - n, x, c))
TO_C = pairs(lambda n, x, c: (n, x, 1 - c))


def permute(value, where):
    return lax.ppermute(value, AXES, where)


def my_place():
    node = lax.axis_index('node')
    local = lax.axis_index('local')
    return node, local // 2, local % 2


def dot_nn(a, b):
    return lax.dot_general(a, b, (((1,), (0,)), ((), ())), preferred_element_type=F32)


def dot_nt(a, b):
    return lax.dot_general(a, b, (((1,), (1,)), ((), ())), preferred_element_type=F32)


def dot_tn(a, b):
    return lax.dot_general(a, b, (((0,), (0,)), ((), ())), preferred_element_type=F32)


def call(kernel, outs, args, flops, scratch=(), specs=None, name=None):
    bytes_all = sum(a.size * a.dtype.itemsize for a in args) + sum(o.size * o.dtype.itemsize for o in outs)
    return pl.pallas_call(
        kernel, out_shape=outs, in_specs=specs or [VMEM] * len(args), out_specs=[VMEM] * len(outs),
        scratch_shapes=list(scratch), name=name,
        cost_estimate=pl.CostEstimate(flops=int(flops), bytes_accessed=int(bytes_all), transcendentals=0),
        compiler_params=pltpu.CompilerParams(vmem_limit_bytes=56 * 1024 * 1024))(*args)


def struct(shape, dtype):
    return jax.ShapeDtypeStruct(shape, dtype)


def gather_pieces(own):
    half = own.shape[0] // 2
    from_x = permute(own, TO_X)
    from_y = permute(own, TO_Y)
    diag_a = permute(from_y[:half], TO_X)
    diag_b = permute(from_x[half:], TO_Y)
    mine = [own, from_x, from_y, diag_a, diag_b]
    return mine + [permute(piece, TO_C) for piece in mine]


def assemble_kernel(*refs):
    pieces, full, sems = refs[:10], refs[10], refs[11]
    node, xpos, core = my_place()
    rows = pieces[0].shape[0]
    half = rows // 2
    copies = []
    for side in range(2):
        cpos = core if side == 0 else 1 - core
        for k, (n, x, off) in enumerate(((node, xpos, 0), (node, 1 - xpos, 0), (1 - node, xpos, 0),
                                         (1 - node, 1 - xpos, 0), (1 - node, 1 - xpos, half))):
            start = pl.multiple_of((n * 4 + x * 2 + cpos) * rows + off, 16)
            idx = side * 5 + k
            size = rows if k < 3 else half
            copies.append(pltpu.make_async_copy(pieces[idx], full.at[pl.ds(start, size), :], sems.at[idx]))
    for copy in copies:
        copy.start()
    for copy in copies:
        copy.wait()


def assemble(pieces):
    rows, cols = pieces[0].shape
    return call(assemble_kernel, [struct((rows * 8, cols), BF)], pieces, 1e9,
                scratch=[pltpu.SemaphoreType.DMA((10,))], specs=[ANY] * 10, name='assemble')[0]


def rotate(block, cos_t, low_t, high_t):
    lanes = block.shape[1]
    return block * cos_t + pltpu.roll(block, lanes - 8, 1) * low_t + pltpu.roll(block, 8, 1) * high_t


def rotate_back(block, cos_t, low_t, high_t):
    lanes = block.shape[1]
    return block * cos_t + pltpu.roll(block * low_t, 8, 1) + pltpu.roll(block * high_t, lanes - 8, 1)


def softmax_rows(scores):
    peak = jnp.max(scores, axis=-1, keepdims=True)
    powers = jnp.exp(scores - peak)
    return powers / jnp.sum(powers, axis=-1, keepdims=True)


def causal_mask(seq):
    return lax.broadcasted_iota(jnp.int32, (seq, seq), 0) >= lax.broadcasted_iota(jnp.int32, (seq, seq), 1)


def attn_fwd_kernel(h_ref, w_ref, sp_ref, qb_ref, cos_ref, low_ref, high_ref,
                    na_ref, nm_ref, qkv_ref, ctx_ref, res_ref):
    tokens, d_model = h_ref.shape
    seq = cos_ref.shape[0]
    heads = d_model // 64

    @pl.loop(0, tokens // seq)
    def _(s):
        rows = pl.ds(pl.multiple_of(s * seq, seq), seq)
        x = h_ref[rows, :].astype(F32)
        center = x - jnp.mean(x, axis=-1, keepdims=True)
        scaled = center * lax.rsqrt(jnp.mean(center * center, axis=-1, keepdims=True) + EPSILON)
        na_ref[rows, :] = (scaled * sp_ref[0:1, :] + sp_ref[1:2, :]).astype(BF)
        nm_ref[rows, :] = (scaled * sp_ref[3:4, :] + sp_ref[4:5, :]).astype(BF)

    @pl.loop(0, 6)
    def _(t):
        cols = pl.ds(pl.multiple_of(t * 384, 384), 384)
        val = dot_nn(na_ref[...], w_ref[:, cols]) + qb_ref[0:1, cols]
        for s in range(tokens // seq):
            piece = val[s * seq:(s + 1) * seq, :]
            qkv_ref[s * seq:(s + 1) * seq, cols] = rotate(piece, cos_ref[...], low_ref[...], high_ref[...]).astype(BF)

    mask = causal_mask(seq)

    @pl.loop(0, tokens // seq)
    def _(s):
        rows = pl.ds(pl.multiple_of(s * seq, seq), seq)
        for pair in range(heads // 2):
            block = qkv_ref[rows, pair * 384:(pair + 1) * 384]
            outs = []
            for i in range(2):
                query = block[:, i * 192:i * 192 + 64]
                key = block[:, i * 192 + 64:i * 192 + 128]
                value = block[:, i * 192 + 128:i * 192 + 192]
                scores = jnp.where(mask, dot_nt(query, key) * 0.125, -1e30)
                probs = softmax_rows(scores).astype(BF)
                outs.append(dot_nn(probs, value).astype(BF))
            ctx_ref[rows, pair * 128:(pair + 1) * 128] = jnp.concatenate(outs, axis=1)

    @pl.loop(0, 3)
    def _(t):
        cols = pl.ds(pl.multiple_of(t * 256, 256), 256)
        wcols = pl.ds(pl.multiple_of(2304 + t * 256, 256), 256)
        res_ref[:, cols] = (h_ref[:, cols].astype(F32)
                            + (dot_nn(ctx_ref[...], w_ref[:, wcols]) + sp_ref[2:3, cols]))


def attn_fwd(h, w_qo, sp, qkv_bias, tables):
    tokens, d_model = h.shape
    outs = [struct((tokens, d_model), BF), struct((tokens, d_model), BF), struct((tokens, 3 * d_model), BF),
            struct((tokens, d_model), BF), struct((tokens, d_model), F32)]
    return call(attn_fwd_kernel, outs, [h, w_qo, sp, qkv_bias, *tables], 2 * tokens * d_model * 4 * d_model * 2,
                name='attn_fwd')


def split_rows(full_t, own_ref, other_ref, rows):
    node, xpos, core = my_place()
    for ry in range(2):
        for rx in range(2):
            n = node if ry == 0 else 1 - node
            x = xpos if rx == 0 else 1 - xpos
            for rc, out in ((0, own_ref), (1, other_ref)):
                c = core if rc == 0 else 1 - core
                start = pl.multiple_of((n * 4 + x * 2 + c) * rows, 16)
                out[(ry * 2 + rx) * rows:(ry * 2 + rx + 1) * rows, :] = full_t[pl.ds(start, rows), :]


def transpose_to(src_ref, dst_ref):
    tokens, width = src_ref.shape

    @pl.loop(0, width // 128)
    def _(t):
        cols = pl.ds(pl.multiple_of(t * 128, 128), 128)
        dst_ref[cols, :] = src_ref[:, cols].T


def attn_bwd_kernel(d_ref, w_ref, qkv_ref, ctx_ref, na_ref, cos_ref, low_ref, high_ref,
                    ctx_own, ctx_oth, na_own, na_oth, dqkv_ref, dna_ref, bsum_ref, dsum_ref,
                    dctx_ref, turn_ref):
    tokens, d_model = d_ref.shape
    seq = cos_ref.shape[0]
    heads = d_model // 64

    @pl.loop(0, 3)
    def _(t):
        cols = pl.ds(pl.multiple_of(t * 256, 256), 256)
        dctx_ref[:, cols] = dot_nt(d_ref[...], w_ref[cols, 2304:3072]).astype(BF)

    transpose_to(ctx_ref, turn_ref)
    split_rows(turn_ref, ctx_own, ctx_oth, d_model // 8)
    transpose_to(na_ref, turn_ref)
    split_rows(turn_ref, na_own, na_oth, d_model // 8)

    bsum_ref[...] = jnp.zeros_like(bsum_ref)
    dsum_ref[...] = jnp.zeros_like(dsum_ref)
    mask = causal_mask(seq)

    @pl.loop(0, tokens // seq)
    def _(s):
        rows = pl.ds(pl.multiple_of(s * seq, seq), seq)
        dsum_ref[...] += jnp.sum(d_ref[rows, :].astype(F32), axis=0, keepdims=True)
        for pair in range(heads // 2):
            block = qkv_ref[rows, pair * 384:(pair + 1) * 384]
            dblock = dctx_ref[rows, pair * 128:(pair + 1) * 128]
            outs = []
            for i in range(2):
                query = block[:, i * 192:i * 192 + 64]
                key = block[:, i * 192 + 64:i * 192 + 128]
                value = block[:, i * 192 + 128:i * 192 + 192]
                dctx = dblock[:, i * 64:(i + 1) * 64]
                scores = jnp.where(mask, dot_nt(query, key) * 0.125, -1e30)
                probs = softmax_rows(scores)
                dprobs = dot_nt(dctx, value).astype(BF).astype(F32)
                dvalue = dot_tn(probs.astype(BF), dctx).astype(BF)
                dscores = (probs * (dprobs - jnp.sum(dprobs * probs, axis=-1, keepdims=True)) * 0.125).astype(BF)
                dquery = dot_nn(dscores, key).astype(BF)
                dkey = dot_tn(dscores, query).astype(BF)
                outs += [dquery, dkey, dvalue]
            turned = rotate_back(jnp.concatenate(outs, axis=1).astype(F32), cos_ref[...], low_ref[...], high_ref[...])
            cols = slice(pair * 384, (pair + 1) * 384)
            bsum_ref[:, cols] += jnp.sum(turned, axis=0, keepdims=True)
            dqkv_ref[rows, cols] = turned.astype(BF)

    @pl.loop(0, 3)
    def _(t):
        cols = pl.ds(pl.multiple_of(t * 256, 256), 256)
        dna_ref[:, cols] = dot_nt(dqkv_ref[...], w_ref[cols, 0:2304]).astype(BF)


def attn_bwd(d_out, w_qo, qkv, ctx, na, tables):
    tokens, d_model = d_out.shape
    half = d_model // 2
    outs = [struct((half, tokens), BF)] * 4 + [struct((tokens, 3 * d_model), BF), struct((tokens, d_model), BF),
                                              struct((1, 3 * d_model), F32), struct((1, d_model), F32)]
    return call(attn_bwd_kernel, outs, [d_out, w_qo, qkv, ctx, na, *tables], 2 * tokens * d_model * 4 * d_model * 3,
                scratch=[pltpu.VMEM((tokens, d_model), BF), pltpu.VMEM((d_model, tokens), BF)], name='attn_bwd')


def mlp_fwd_kernel(nm_ref, up_ref, ub_ref, down_ref, db_ref, res_ref, out_ref, act_ref):
    tokens, d_model = nm_ref.shape
    hidden = up_ref.shape[1]

    @pl.loop(0, hidden // 384)
    def _(t):
        cols = pl.ds(pl.multiple_of(t * 384, 384), 384)
        pre = dot_nn(nm_ref[...], up_ref[:, cols]) + ub_ref[0:1, cols]
        act_ref[:, cols] = (0.5 * pre * (1.0 + lax.erf(pre * SQRT_HALF))).astype(BF)

    @pl.loop(0, d_model // 256)
    def _(t):
        cols = pl.ds(pl.multiple_of(t * 256, 256), 256)
        out_ref[:, cols] = (res_ref[:, cols] + (dot_nn(act_ref[...], down_ref[:, cols]) + db_ref[0:1, cols])).astype(BF)


def mlp_fwd(nm, w_up, up_bias, w_down, down_bias, res):
    tokens, d_model = nm.shape
    return call(mlp_fwd_kernel, [struct((tokens, d_model), BF)], [nm, w_up, up_bias, w_down, down_bias, res],
                4 * tokens * d_model * w_up.shape[1], scratch=[pltpu.VMEM((tokens, w_up.shape[1]), BF)], name='mlp_fwd')[0]


def mlp_bwd_kernel(with_out, *refs):
    nm_ref, d_ref, up_ref, ub_ref, down_ref = refs[:5]
    refs = refs[5:]
    if with_out:
        db_ref, res_ref = refs[:2]
        refs = refs[2:]
    act_own, act_oth, nm_own, nm_oth, dpre_ref, dnm_ref, ubsum_ref = refs[:7]
    refs = refs[7:]
    if with_out:
        out_ref, sum_ref, turn_ref = refs
    else:
        turn_ref, = refs
    tokens, d_model = nm_ref.shape
    node, xpos, core = my_place()
    block = 384

    transpose_to(nm_ref, turn_ref)
    split_rows(turn_ref, nm_own, nm_oth, d_model // 8)
    if with_out:
        sum_ref[...] = res_ref[...] + db_ref[...]

    def step(n, x, c, slot, out):
        start = pl.multiple_of((n * 4 + x * 2 + c) * block, block)
        cols = pl.ds(start, block)
        pre = dot_nn(nm_ref[...], up_ref[:, cols]) + ub_ref[0:1, cols]
        dact = dot_nt(d_ref[...], down_ref[cols, :]).astype(BF).astype(F32)
        cdf = 0.5 * (1.0 + lax.erf(pre * SQRT_HALF))
        act = (pre * cdf).astype(BF)
        dpre = dact * (cdf + pre * (jnp.exp(-0.5 * pre * pre) * INV_SQRT_2PI))
        ubsum_ref[0:1, cols] = jnp.sum(dpre, axis=0, keepdims=True)
        dpre_ref[:, cols] = dpre.astype(BF)
        out[pl.ds(pl.multiple_of(slot * block, block), block), :] = act.T
        if with_out:
            sum_ref[...] += dot_nn(act, down_ref[cols, :])

    @pl.loop(0, 4)
    def _(t):
        ry, rx = t // 2, t % 2
        n = (node + ry) % 2
        x = (xpos + rx) % 2
        step(n, x, core, t, act_own)
        step(n, x, 1 - core, t, act_oth)

    @pl.loop(0, d_model // 256)
    def _(t):
        cols = pl.ds(pl.multiple_of(t * 256, 256), 256)
        dnm_ref[:, cols] = dot_nt(dpre_ref[...], up_ref[cols, :]).astype(BF)
    if with_out:
        out_ref[...] = sum_ref[...].astype(BF)


def mlp_bwd(nm, d_out, w_up, up_bias, w_down, down_bias=None, res=None):
    tokens, d_model = nm.shape
    hidden = w_up.shape[1]
    with_out = res is not None
    outs = [struct((hidden // 2, tokens), BF)] * 2 + [struct((d_model // 2, tokens), BF)] * 2
    outs += [struct((tokens, hidden), BF), struct((tokens, d_model), BF), struct((1, hidden), F32)]
    args = [nm, d_out, w_up, up_bias, w_down]
    scratch = [pltpu.VMEM((d_model, tokens), BF)]
    if with_out:
        args += [down_bias, res]
        outs += [struct((tokens, d_model), BF)]
        scratch = [pltpu.VMEM((tokens, d_model), F32)] + scratch
    return call(functools.partial(mlp_bwd_kernel, with_out), outs, args, 2 * tokens * d_model * hidden * (4 if with_out else 3),
                scratch=scratch, name='mlp_bwd')


def norm_bwd_kernel(h_ref, d_ref, dna_ref, dnm_ref, sp_ref, dh_ref, sums_ref):
    tokens, d_model = h_ref.shape
    sums_ref[...] = jnp.zeros_like(sums_ref)

    @pl.loop(0, tokens // 128)
    def _(s):
        rows = pl.ds(pl.multiple_of(s * 128, 128), 128)
        x = h_ref[rows, :].astype(F32)
        center = x - jnp.mean(x, axis=-1, keepdims=True)
        inv = lax.rsqrt(jnp.mean(center * center, axis=-1, keepdims=True) + EPSILON)
        scaled = center * inv
        da = dna_ref[rows, :].astype(F32)
        dm = dnm_ref[rows, :].astype(F32)
        sums_ref[0:1, :] += jnp.sum(da * scaled, axis=0, keepdims=True)
        sums_ref[1:2, :] += jnp.sum(da, axis=0, keepdims=True)
        sums_ref[2:3, :] += jnp.sum(dm * scaled, axis=0, keepdims=True)
        sums_ref[3:4, :] += jnp.sum(dm, axis=0, keepdims=True)
        dscaled = da * sp_ref[0:1, :] + dm * sp_ref[3:4, :]
        dh = inv * (dscaled - jnp.mean(dscaled, axis=-1, keepdims=True)
                    - scaled * jnp.mean(dscaled * scaled, axis=-1, keepdims=True))
        dh_ref[rows, :] = (d_ref[rows, :].astype(F32) + dh).astype(BF)


def norm_bwd(h, d_out, dna, dnm, sp):
    tokens, d_model = h.shape
    return call(norm_bwd_kernel, [struct((tokens, d_model), BF), struct((8, d_model), F32)],
                [h, d_out, dna, dnm, sp], 2e9, name='norm_bwd')


def grad_kernel(first, tile, xo_ref, xr_ref, yo_ref, yr_ref, a_ref, b_ref):
    rows = xo_ref.shape[0] // 4
    half = yo_ref.shape[1] // 2
    a_sel = (1, 3) if first else (0, 2)
    b_sel = (2, 3) if first else (0, 1)
    for sel, out, base in ((a_sel, a_ref, 0), (b_sel, b_ref, half)):
        own = jnp.concatenate([xo_ref[k * rows:(k + 1) * rows, :] for k in sel], axis=0)
        rcv = jnp.concatenate([xr_ref[k * rows:(k + 1) * rows, :] for k in sel], axis=0)

        @pl.loop(0, half // tile)
        def _(t):
            cols = pl.ds(pl.multiple_of(base + t * tile, 128), tile)
            ocols = pl.ds(pl.multiple_of(t * tile, 128), tile)
            out[:, ocols] = dot_nn(own, yo_ref[:, cols]) + dot_nn(rcv, yr_ref[:, cols])


def grad_half(first, xo, xr, yo, yr):
    rows, half = xo.shape[0] // 2, yo.shape[1] // 2
    outs = [struct((rows, half), F32)] * 2
    return call(functools.partial(grad_kernel, first, 384), outs, [xo, xr, yo, yr],
                4 * xo.shape[0] * xo.shape[1] * yo.shape[1] // 2, name='grad_half')


def weight_grad(x_own, x_oth, y):
    x_rcv = permute(x_oth, TO_C)
    y_rcv = permute(y, TO_C)
    a_send, b_send = grad_half(True, x_own, x_rcv, y, y_rcv)
    a_got = permute(a_send, TO_X)
    b_got = permute(b_send, TO_Y)
    a_keep, b_keep = grad_half(False, x_own, x_rcv, y, y_rcv)
    rows = a_keep.shape[0] // 2
    a_more = permute(a_keep[rows:] + a_got[rows:], TO_Y)
    b_more = permute(b_keep[rows:] + b_got[rows:], TO_X)
    a_sum = a_keep[:rows] + a_got[:rows] + a_more
    b_sum = b_keep[:rows] + b_got[:rows] + b_more
    return jnp.concatenate([a_sum, b_sum], axis=1).astype(BF)


def rope_tables(seq, width):
    lane = jnp.arange(384) % 192
    turned = (lane < 128) & (lane % 64 < 16)
    inv_freq = 1.0 / (10000.0 ** (jnp.arange(0, 16, 2, dtype=F32) / 16))
    angles = jnp.arange(seq, dtype=F32)[:, None] * inv_freq[None, :]
    angles = jnp.tile(angles, (1, 48))
    low = turned & (lane % 16 < 8)
    high = turned & (lane % 16 >= 8)
    cos_t = jnp.where(turned, jnp.cos(angles), 1.0)
    low_t = jnp.where(low, -jnp.sin(angles), 0.0)
    high_t = jnp.where(high, jnp.sin(angles), 0.0)
    return cos_t, low_t, high_t


def small_params(shards):
    packed = jnp.concatenate(shards, axis=1)
    full = lax.all_gather(packed, AXES).astype(F32)
    out = []
    for layer in range(2):
        part = full[:, layer]
        pos = 0
        rows = []
        for shard in shards:
            width = shard.shape[1]
            rows.append(part[:, pos:pos + width].reshape(1, -1))
            pos += width
        out.append(rows)
    return out


def device_step(x, y_cot, ln1_g, ln1_b, qkv_w, qkv_b, out_w, out_b, ln2_g, ln2_b, up_w, up_b, down_w, down_b):
    batch, seq, d_model = x.shape
    tokens = batch * seq
    layers = range(2)
    qkv_flat = qkv_w.reshape(2, qkv_w.shape[1], -1)
    chunks = []
    for i in layers:
        for own in (jnp.concatenate([qkv_flat[i], out_w[i]], axis=1), up_w[i], down_w[i]):
            chunks.append(gather_pieces(own))
    smalls = small_params([ln1_g, ln1_b, qkv_b, out_b, ln2_g, ln2_b, up_b, down_b])
    sps = [jnp.concatenate([r[0], r[1], r[3], r[4], r[5], r[7], r[7], r[7]], axis=0) for r in smalls]
    qbs = [r[2] for r in smalls]
    ubs = [r[6] for r in smalls]
    dbs = [r[7] for r in smalls]
    tables = rope_tables(seq, 384)
    weights = [assemble(pieces) for pieces in chunks]
    qo, up, down = weights[0::3], weights[1::3], weights[2::3]

    h0 = x.reshape(tokens, d_model)
    cot = y_cot.reshape(tokens, d_model)
    na0, nm0, qkv0, ctx0, res0 = attn_fwd(h0, qo[0], sps[0], qbs[0], tables)
    h1 = mlp_fwd(nm0, up[0], ubs[0], down[0], dbs[0], res0)
    na1, nm1, qkv1, ctx1, res1 = attn_fwd(h1, qo[1], sps[1], qbs[1], tables)

    grads = [None, None]

    def attn_back(i, d_out, qkv, ctx, na):
        c_own, c_oth, n_own, n_oth, dqkv, dna, qsum, dsum = attn_bwd(d_out, qo[i], qkv, ctx, na, tables)
        return dna, qsum, dsum, weight_grad(c_own, c_oth, d_out), weight_grad(n_own, n_oth, dqkv)

    dna1, qsum1, dsum1, gout1, gqkv1 = attn_back(1, cot, qkv1, ctx1, na1)
    a_own, a_oth, m_own, m_oth, dpre, dnm1, usum1, y_out = mlp_bwd(nm1, cot, up[1], ubs[1], down[1], dbs[1], res1)
    gdown1 = weight_grad(a_own, a_oth, cot)
    gup1 = weight_grad(m_own, m_oth, dpre)
    d1, sums1 = norm_bwd(h1, cot, dna1, dnm1, sps[1])

    a_own, a_oth, m_own, m_oth, dpre, dnm0, usum0 = mlp_bwd(nm0, d1, up[0], ubs[0], down[0])
    gdown0 = weight_grad(a_own, a_oth, d1)
    gup0 = weight_grad(m_own, m_oth, dpre)
    dna0, qsum0, dsum0, gout0, gqkv0 = attn_back(0, d1, qkv0, ctx0, na0)
    x_grad, sums0 = norm_bwd(h0, d1, dna0, dnm0, sps[0])

    packs = []
    for sums, qsum, dsum, usum in ((sums0, qsum0, dsum0, usum0), (sums1, qsum1, dsum1, usum1)):
        pieces = [sums[0:1], sums[1:2], qsum, dsum, sums[2:3], sums[3:4], usum]
        packs.append(jnp.concatenate([p.reshape(8, -1) for p in pieces], axis=1))
    small = lax.psum_scatter(jnp.concatenate(packs, axis=1), AXES, scatter_dimension=0, tiled=True)
    small = small.reshape(2, -1)
    small = small.astype(BF)
    cuts = []
    pos = 0
    for width in (96, 96, 288, 96, 96, 96, 384):
        cuts.append(small[:, pos:pos + width])
        pos += width
    g1, b1, qb, ob, g2, b2, ub = cuts
    gqkv = jnp.stack([gqkv0, gqkv1]).reshape(qkv_w.shape)
    return (y_out.reshape(x.shape), x_grad.reshape(x.shape), g1, b1, gqkv, qb, jnp.stack([gout0, gout1]), ob,
            g2, b2, jnp.stack([gup0, gup1]), ub, jnp.stack([gdown0, gdown1]), ob)


def solution(mesh):
    act_spec = P(AXES)
    param_spec = P(None, AXES)
    return jax.shard_map(device_step, mesh=mesh, in_specs=(act_spec, act_spec) + (param_spec,) * 12,
                         out_specs=(act_spec, act_spec) + (param_spec,) * 12, check_vma=False)
```

```python
import functools
import jax
import jax.numpy as jnp
from jax import lax
from jax.experimental import pallas as pl
from jax.experimental.pallas import tpu as pltpu
from jax.sharding import PartitionSpec as P

EPSILON = 1e-5
BF = jnp.bfloat16
F32 = jnp.float32
AXES = ('node', 'local')
SQRT_HALF = 0.7071067811865476
INV_SQRT_2PI = 0.3989422804014327
VMEM = pl.BlockSpec(memory_space=pltpu.VMEM)
ANY = pl.BlockSpec(memory_space=pl.ANY)


def pairs(move):
    out = []
    for n in range(2):
        for x in range(2):
            for c in range(2):
                n2, x2, c2 = move(n, x, c)
                out.append((n * 4 + x * 2 + c, n2 * 4 + x2 * 2 + c2))
    return out


TO_X = pairs(lambda n, x, c: (n, 1 - x, c))
TO_Y = pairs(lambda n, x, c: (1 - n, x, c))
TO_C = pairs(lambda n, x, c: (n, x, 1 - c))


def permute(value, where):
    return lax.ppermute(value, AXES, where)


def my_place():
    node = lax.axis_index('node')
    local = lax.axis_index('local')
    return node, local // 2, local % 2


def dot_nn(a, b):
    return lax.dot_general(a, b, (((1,), (0,)), ((), ())), preferred_element_type=F32)


def dot_nt(a, b):
    return lax.dot_general(a, b, (((1,), (1,)), ((), ())), preferred_element_type=F32)


def dot_tn(a, b):
    return lax.dot_general(a, b, (((0,), (0,)), ((), ())), preferred_element_type=F32)


def call(kernel, outs, args, flops, scratch=(), specs=None, grid=(), out_specs=None, room=0):
    bytes_all = sum(a.size * a.dtype.itemsize for a in args) + sum(o.size * o.dtype.itemsize for o in outs)
    room = room or int(bytes_all / 2**20) + 14
    return pl.pallas_call(
        kernel, out_shape=outs, in_specs=specs or [VMEM] * len(args), out_specs=out_specs or [VMEM] * len(outs), grid=grid,
        scratch_shapes=list(scratch),
        cost_estimate=pl.CostEstimate(flops=int(flops), bytes_accessed=int(bytes_all), transcendentals=0),
        compiler_params=pltpu.CompilerParams(vmem_limit_bytes=room * 1024 * 1024))(*args)


def struct(shape, dtype):
    return jax.ShapeDtypeStruct(shape, dtype)


SMALL_WIDTHS = (96, 96, 288, 96, 96, 96, 384, 96)


def gather_near(own):
    return own, permute(own, TO_X), permute(own, TO_Y)


def gather_pieces(near, half, late=None):
    own, from_x, from_y = near
    if late is not None:
        from_x, from_y = after(from_x, late), after(from_y, late)
    diag_a = permute(from_y[:half], TO_X)
    diag_b = permute(from_x[half:], TO_Y)
    mine = [own, from_x, from_y, diag_a, diag_b]
    return mine + [permute(piece, TO_C) for piece in mine]


def piece_places(rows):
    node, xpos, core = my_place()
    half = rows // 2
    out = []
    for side in range(2):
        cpos = core if side == 0 else 1 - core
        for k, (n, x, off, size) in enumerate(((node, xpos, 0, rows), (node, 1 - xpos, 0, rows), (1 - node, xpos, 0, rows),
                                               (1 - node, 1 - xpos, 0, half), (1 - node, 1 - xpos, half, half))):
            out.append((side * 5 + k, n * 4 + x * 2 + cpos, off, size))
    return out


def run_copies(copies):
    for copy in copies:
        copy.start()
    for copy in copies:
        copy.wait()


def regroup(line, outer, inner):
    starts = [base + (o * inner + i) * 64 for base in range(0, 2304, 384) for i in range(inner) for o in range(outer)]
    return jnp.concatenate([line[:, t:t + 64] for t in starts], axis=1)


def assemble_qo_kernel(*refs):
    pieces, full, small_ref, raw, sems = refs[:10], refs[10], refs[11], refs[12], refs[13]
    copies = []
    for idx, dev, off, size in piece_places(96):
        copies.append(pltpu.make_async_copy(
            pieces[idx].at[pl.ds(0, size), :], full.at[pl.ds(pl.multiple_of(dev * 96 + off, 16), size), :], sems.at[idx]))
        if off + size == 96:
            copies.append(pltpu.make_async_copy(
                pieces[idx].at[pl.ds(size, 16), :], raw.at[pl.ds(pl.multiple_of(dev * 16, 16), 16), :], sems.at[10 + idx]))
    run_copies(copies)
    for layer in range(2):
        rows = jnp.concatenate([raw[j * 16:(j + 1) * 16, :].astype(F32)[layer:layer + 1, :] for j in range(8)], axis=0)
        pos = 0
        for k, width in enumerate(SMALL_WIDTHS):
            line = jnp.concatenate([rows[j:j + 1, pos:pos + width] for j in range(8)], axis=1)
            if width == 288:
                line = regroup(line, 2, 3)
            small_ref[layer * 8 + k:layer * 8 + k + 1, 0:8 * width] = line
            pos += width


def assemble_qo(pieces):
    return call(assemble_qo_kernel, [struct((768, 3072), BF), struct((16, 3072), F32)], pieces, 1e9,
            scratch=[pltpu.VMEM((128, 3072), BF), pltpu.SemaphoreType.DMA((20,))], specs=[ANY] * 10)


def assemble_kernel(*refs):
    pieces, full, sems = refs[:10], refs[10], refs[11]
    rows = full.shape[0] // 8
    run_copies([pltpu.make_async_copy(
        pieces[idx], full.at[pl.ds(pl.multiple_of(dev * rows + off, 16), size), :], sems.at[idx])
        for idx, dev, off, size in piece_places(rows)])


def assemble(pieces):
    rows, cols = pieces[0].shape
    return call(assemble_kernel, [struct((rows * 8, cols), BF)], pieces, 1e9,
                scratch=[pltpu.SemaphoreType.DMA((10,))], specs=[ANY] * 10)[0]


def rotate(block, cos_t, low_t, high_t):
    return block * cos_t + pltpu.roll(block, 120, 1) * low_t + pltpu.roll(block, 8, 1) * high_t


def rotate_back(block, cos_t, low_t, high_t):
    return block * cos_t + pltpu.roll(block * low_t, 8, 1) + pltpu.roll(block * high_t, 120, 1)


def softmax_down(scores):
    peak = jnp.max(scores, axis=0, keepdims=True)
    powers = jnp.exp(scores - peak)
    return powers * (1.0 / jnp.sum(powers, axis=0, keepdims=True))


def paired_mask(seq):
    keys = lax.broadcasted_iota(jnp.int32, (seq, seq), 0)
    queries = lax.broadcasted_iota(jnp.int32, (seq, seq), 1)
    return jnp.concatenate([queries >= keys] * 2, axis=1)


def by_head(block, left):
    zero = jnp.zeros_like(block)
    return jnp.concatenate([jnp.where(left, block, zero), jnp.where(left, zero, block)], axis=0)


def join_heads(stacked, left):
    rows = stacked.shape[0] // 2
    return jnp.where(left, stacked[:rows], stacked[rows:])


def attn_fwd_kernel(layer, h_ref, w_ref, small_ref, cos_ref, low_ref, high_ref,
                    na_ref, nm_ref, qkv_ref, ctx_ref, res_ref):
    tokens, d_model = h_ref.shape
    seq = cos_ref.shape[0]
    heads = d_model // 64

    def small(k, cols=slice(0, 768)):
        return small_ref[layer * 8 + k:layer * 8 + k + 1, cols]

    @pl.loop(0, tokens // seq)
    def _(s):
        rows = pl.ds(pl.multiple_of(s * seq, seq), seq)
        x = h_ref[rows, :].astype(F32)
        center = x - jnp.mean(x, axis=-1, keepdims=True)
        scaled = center * lax.rsqrt(jnp.mean(center * center, axis=-1, keepdims=True) + EPSILON)
        na_ref[rows, :] = (scaled * small(0) + small(1)).astype(BF)
        nm_ref[rows, :] = (scaled * small(4) + small(5)).astype(BF)

    @pl.loop(0, 3)
    def _(t):
        cols = pl.ds(pl.multiple_of(t * 768, 768), 768)
        val = dot_nn(na_ref[...], w_ref[:, cols]) + small(2, cols)
        for s in range(tokens // seq):
            rows = slice(s * seq, (s + 1) * seq)
            for part in range(6):
                piece = val[rows, part * 128:(part + 1) * 128]
                if part % 3 < 2:
                    piece = rotate(piece, cos_ref[...], low_ref[...], high_ref[...])
                qkv_ref[rows, pl.ds(pl.multiple_of(t * 768 + part * 128, 128), 128)] = piece.astype(BF)

    mask = paired_mask(seq)
    left = lax.broadcasted_iota(jnp.int32, (seq, 128), 1) < 64

    @pl.loop(0, tokens // seq)
    def _(s):
        rows = pl.ds(pl.multiple_of(s * seq, seq), seq)
        for pair in range(heads // 2):
            base = pair * 384
            query = by_head(qkv_ref[rows, base:base + 128], left)
            key = qkv_ref[rows, base + 128:base + 256]
            value = qkv_ref[rows, base + 256:base + 384]
            scores = jnp.where(mask, dot_nt(key, query) * 0.125, -1e30)
            probs = softmax_down(scores).astype(BF)
            ctx_ref[rows, pair * 128:(pair + 1) * 128] = join_heads(dot_tn(probs, value), left).astype(BF)

    @pl.loop(0, 3)
    def _(t):
        cols = pl.ds(pl.multiple_of(t * 256, 256), 256)
        wcols = pl.ds(pl.multiple_of(2304 + t * 256, 256), 256)
        res_ref[:, cols] = (h_ref[:, cols].astype(F32)
                            + (dot_nn(ctx_ref[...], w_ref[:, wcols]) + small(3, cols)))


def attn_fwd(layer, h, w_qo, small, tables):
    tokens, d_model = h.shape
    outs = [struct((tokens, d_model), BF), struct((tokens, d_model), BF), struct((tokens, 3 * d_model), BF),
            struct((tokens, d_model), BF), struct((tokens, d_model), F32)]
    return call(functools.partial(attn_fwd_kernel, layer), outs, [h, w_qo, small, *tables], 20e9)


def split_rows(full_t, own_ref, other_ref, rows, base=0):
    node, xpos, core = my_place()
    for ry in range(2):
        for rx in range(2):
            n = node if ry == 0 else 1 - node
            x = xpos if rx == 0 else 1 - xpos
            for rc, out in ((0, own_ref), (1, other_ref)):
                c = core if rc == 0 else 1 - core
                start = pl.multiple_of((n * 4 + x * 2 + c) * rows, 16)
                first = base + (ry * 2 + rx) * rows
                out[first:first + rows, :] = full_t[pl.ds(start, rows), :]


def transpose_to(src_ref, dst_ref):
    _, width = src_ref.shape

    @pl.loop(0, width // 128)
    def _(t):
        cols = pl.ds(pl.multiple_of(t * 128, 128), 128)
        dst_ref[cols, :] = src_ref[:, cols].T


def attn_bwd_kernel(d_ref, w_ref, qkv_ref, ctx_ref, na_ref, cos_ref, low_ref, high_ref,
                    x_own, x_oth, dqkv_ref, bsum_ref, dsum_ref, dctx_ref, turn_ref):
    tokens, d_model = d_ref.shape
    seq = cos_ref.shape[0]
    heads = d_model // 64

    @pl.loop(0, 3)
    def _(t):
        cols = pl.ds(pl.multiple_of(t * 256, 256), 256)
        dctx_ref[:, cols] = dot_nt(d_ref[...], w_ref[cols, 2304:3072]).astype(BF)

    transpose_to(ctx_ref, turn_ref)
    split_rows(turn_ref, x_own, x_oth, d_model // 8)
    transpose_to(na_ref, turn_ref)
    split_rows(turn_ref, x_own, x_oth, d_model // 8, d_model // 2)

    bsum_ref[...] = jnp.zeros_like(bsum_ref)
    dsum_ref[...] = jnp.zeros_like(dsum_ref)
    mask = paired_mask(seq)
    left = lax.broadcasted_iota(jnp.int32, (seq, 128), 1) < 64

    @pl.loop(0, tokens // seq)
    def _(s):
        rows = pl.ds(pl.multiple_of(s * seq, seq), seq)
        dsum_ref[...] += jnp.sum(d_ref[rows, :].astype(F32), axis=0, keepdims=True)
        for pair in range(heads // 2):
            base = pair * 384
            query = by_head(qkv_ref[rows, base:base + 128], left)
            key = qkv_ref[rows, base + 128:base + 256]
            value = qkv_ref[rows, base + 256:base + 384]
            dctx = by_head(dctx_ref[rows, pair * 128:(pair + 1) * 128], left)
            scores = jnp.where(mask, dot_nt(key, query) * 0.125, -1e30)
            probs = softmax_down(scores)
            dprobs = dot_nt(value, dctx).astype(BF).astype(F32)
            dvalue = dot_nn(probs.astype(BF), dctx).astype(BF)
            dscores = (probs * (dprobs - jnp.sum(dprobs * probs, axis=0, keepdims=True)) * 0.125).astype(BF)
            dquery = join_heads(dot_tn(dscores, key), left).astype(BF)
            dkey = dot_nn(dscores, query).astype(BF)
            for part, piece in enumerate((dquery, dkey, dvalue)):
                turned = piece.astype(F32)
                if part < 2:
                    turned = rotate_back(turned, cos_ref[...], low_ref[...], high_ref[...])
                cols = slice(base + part * 128, base + part * 128 + 128)
                bsum_ref[:, cols] += jnp.sum(turned, axis=0, keepdims=True)
                dqkv_ref[rows, cols] = turned.astype(BF)


def attn_bwd(d_out, w_qo, qkv, ctx, na, tables):
    tokens, d_model = d_out.shape
    outs = [struct((d_model, tokens), BF)] * 2 + [struct((tokens, 3 * d_model), BF),
                                                 struct((1, 3 * d_model), F32), struct((1, d_model), F32)]
    return call(attn_bwd_kernel, outs, [d_out, w_qo, qkv, ctx, na, *tables], 25e9,
                scratch=[pltpu.VMEM((tokens, d_model), BF), pltpu.VMEM((d_model, tokens), BF)])


def norm_in_kernel(dqkv_ref, w_ref, dna_ref):
    @pl.loop(0, 3)
    def _(t):
        cols = pl.ds(pl.multiple_of(t * 256, 256), 256)
        dna_ref[:, cols] = dot_nt(dqkv_ref[...], w_ref[cols, 0:2304]).astype(BF)


def attn_in_bwd(dqkv, w_qo):
    tokens, d_model = dqkv.shape[0], w_qo.shape[0]
    return call(norm_in_kernel, [struct((tokens, d_model), BF)], [dqkv, w_qo], 6e9)[0]


def mlp_fwd_kernel(layer, nm_ref, up_ref, down_ref, small_ref, res_ref, out_ref, act_ref):
    _, d_model = nm_ref.shape
    hidden = up_ref.shape[1]

    @pl.loop(0, hidden // 512)
    def _(t):
        cols = pl.ds(pl.multiple_of(t * 512, 512), 512)
        pre = dot_nn(nm_ref[...], up_ref[:, cols]) + small_ref[layer * 8 + 6:layer * 8 + 7, cols]
        act_ref[:, cols] = (0.5 * pre * (1.0 + lax.erf(pre * SQRT_HALF))).astype(BF)

    @pl.loop(0, d_model // 256)
    def _(t):
        cols = pl.ds(pl.multiple_of(t * 256, 256), 256)
        out_ref[:, cols] = (res_ref[:, cols] + (dot_nn(act_ref[...], down_ref[:, cols]) + small_ref[layer * 8 + 7:layer * 8 + 8, cols])).astype(BF)


def mlp_fwd(layer, nm, w_up, w_down, small, res):
    tokens, d_model = nm.shape
    return call(functools.partial(mlp_fwd_kernel, layer), [struct((tokens, d_model), BF)], [nm, w_up, w_down, small, res],
                4 * tokens * d_model * w_up.shape[1], scratch=[pltpu.VMEM((tokens, w_up.shape[1]), BF)])[0]


def mlp_bwd_kernel(layer, with_out, *refs):
    nm_ref, d_ref, up_ref, down_ref, small_ref = refs[:5]
    refs = refs[5:]
    if with_out:
        res_ref = refs[0]
        refs = refs[1:]
    act_own, act_oth, nm_own, nm_oth, dpre_ref, dnm_ref, ubsum_ref = refs[:7]
    refs = refs[7:]
    if with_out:
        out_ref, sum_ref, turn_ref = refs
    else:
        turn_ref, = refs
    _, d_model = nm_ref.shape
    node, xpos, core = my_place()
    block = 384

    transpose_to(nm_ref, turn_ref)
    split_rows(turn_ref, nm_own, nm_oth, d_model // 8)
    if with_out:
        sum_ref[...] = res_ref[...] + small_ref[layer * 8 + 7:layer * 8 + 8, 0:768]

    @pl.loop(0, 4)
    def _(t):
        n = (node + t // 2) % 2
        x = (xpos + t % 2) % 2
        cols = pl.ds(pl.multiple_of((n * 4 + x * 2) * block, 2 * block), 2 * block)
        pre = dot_nn(nm_ref[...], up_ref[:, cols]) + small_ref[layer * 8 + 6:layer * 8 + 7, cols]
        dact = dot_nt(d_ref[...], down_ref[cols, :]).astype(BF).astype(F32)
        cdf = 0.5 * (1.0 + lax.erf(pre * SQRT_HALF))
        act = (pre * cdf).astype(BF)
        dpre = dact * (cdf + pre * (jnp.exp(-0.5 * pre * pre) * INV_SQRT_2PI))
        ubsum_ref[0:1, cols] = jnp.sum(dpre, axis=0, keepdims=True)
        dpre_ref[:, cols] = dpre.astype(BF)
        place = pl.ds(pl.multiple_of(t * block, block), block)
        for c in range(2):
            @pl.when(core == c)
            def _():
                act_own[place, :] = act[:, c * block:(c + 1) * block].T

            @pl.when(core != c)
            def _():
                act_oth[place, :] = act[:, c * block:(c + 1) * block].T
        if with_out:
            sum_ref[...] += dot_nn(act, down_ref[cols, :])

    @pl.loop(0, d_model // 256)
    def _(t):
        cols = pl.ds(pl.multiple_of(t * 256, 256), 256)
        dnm_ref[:, cols] = dot_nt(dpre_ref[...], up_ref[cols, :]).astype(BF)

    if with_out:
        out_ref[...] = sum_ref[...].astype(BF)


def mlp_bwd(layer, nm, d_out, w_up, w_down, small, res=None):
    tokens, d_model = nm.shape
    hidden = w_up.shape[1]
    with_out = res is not None
    outs = [struct((hidden // 2, tokens), BF)] * 2 + [struct((d_model // 2, tokens), BF)] * 2
    outs += [struct((tokens, hidden), BF), struct((tokens, d_model), BF), struct((1, hidden), F32)]
    args = [nm, d_out, w_up, w_down, small]
    scratch = [pltpu.VMEM((d_model, tokens), BF)]
    if with_out:
        args += [res]
        outs += [struct((tokens, d_model), BF)]
        scratch = [pltpu.VMEM((tokens, d_model), F32)] + scratch
    return call(functools.partial(mlp_bwd_kernel, layer, with_out), outs, args,
                2 * tokens * d_model * hidden * (4 if with_out else 3), scratch=scratch)


def norm_bwd_kernel(layer, h_ref, d_ref, dna_ref, dnm_ref, small_ref, dh_ref, sums_ref):
    tokens, _ = h_ref.shape
    sums_ref[...] = jnp.zeros_like(sums_ref)

    @pl.loop(0, tokens // 128)
    def _(s):
        rows = pl.ds(pl.multiple_of(s * 128, 128), 128)
        x = h_ref[rows, :].astype(F32)
        center = x - jnp.mean(x, axis=-1, keepdims=True)
        inv = lax.rsqrt(jnp.mean(center * center, axis=-1, keepdims=True) + EPSILON)
        scaled = center * inv
        da = dna_ref[rows, :].astype(F32)
        dm = dnm_ref[rows, :].astype(F32)
        sums_ref[0:1, :] += jnp.sum(da * scaled, axis=0, keepdims=True)
        sums_ref[1:2, :] += jnp.sum(da, axis=0, keepdims=True)
        sums_ref[2:3, :] += jnp.sum(dm * scaled, axis=0, keepdims=True)
        sums_ref[3:4, :] += jnp.sum(dm, axis=0, keepdims=True)
        dscaled = da * small_ref[layer * 8:layer * 8 + 1, 0:768] + dm * small_ref[layer * 8 + 4:layer * 8 + 5, 0:768]
        dh = inv * (dscaled - jnp.mean(dscaled, axis=-1, keepdims=True)
                    - scaled * jnp.mean(dscaled * scaled, axis=-1, keepdims=True))
        dh_ref[rows, :] = (d_ref[rows, :].astype(F32) + dh).astype(BF)


def norm_bwd(layer, h, d_out, dna, dnm, small):
    tokens, d_model = h.shape
    return call(functools.partial(norm_bwd_kernel, layer), [struct((tokens, d_model), BF), struct((8, d_model), F32)],
                [h, d_out, dna, dnm, small], 4e9)


def product_of_both(xo, xr, yo, yr):
    return dot_nn(xo, yo) + dot_nn(xr, yr)


def put_columns(acc, t, half_tiles, a_send, a_keep, b_send, b_keep):
    rows = acc.shape[0] // 4

    @pl.when(t < half_tiles)
    def _():
        for k, (out, pos) in enumerate(((a_keep, 0), (a_send, 0), (a_keep, 1), (a_send, 1))):
            out[pos * rows:(pos + 1) * rows, :] = acc[k * rows:(k + 1) * rows, :]

    @pl.when(t >= half_tiles)
    def _():
        for k, (out, pos) in enumerate(((b_keep, 0), (b_keep, 1), (b_send, 0), (b_send, 1))):
            out[pos * rows:(pos + 1) * rows, :] = acc[k * rows:(k + 1) * rows, :]


def column_outs(rows, cols, tile, half_tiles):
    left = pl.BlockSpec((rows, tile), lambda t: (0, jnp.minimum(t, half_tiles - 1)))
    right = pl.BlockSpec((rows, tile), lambda t: (0, jnp.maximum(t - half_tiles, 0)))
    return [struct((rows, cols), F32)] * 4, [left, left, right, right]


def grad_up_kernel(xo, xr, yo, yr, *outs):
    put_columns(product_of_both(xo[...], xr[...], yo[...], yr[...]), pl.program_id(0), 3, *outs)


def grad_up(xo, xr, yo, yr):
    tokens = xo.shape[1]
    outs, out_specs = column_outs(192, 1536, 512, 3)
    whole = pl.BlockSpec((384, tokens), lambda t: (0, 0))
    cols = pl.BlockSpec((tokens, 512), lambda t: (0, t))
    return call(grad_up_kernel, outs, [xo, xr, yo, yr], 4e9, specs=[whole, whole, cols, cols], grid=(6,),
                out_specs=out_specs)


def grad_qo_kernel(xo, xr, yo, yr, do, dr, *outs):
    t = pl.program_id(0)
    from_out = (t == 5) | (t >= 10)

    @pl.when(from_out)
    def _():
        put_columns(product_of_both(xo[0:384, :], xr[0:384, :], do[...], dr[...]), t, 6, *outs)

    @pl.when(jnp.logical_not(from_out))
    def _():
        put_columns(product_of_both(xo[384:768, :], xr[384:768, :], yo[...], yr[...]), t, 6, *outs)


def grad_qo(xo, xr, yo, yr, do, dr):
    tokens = xo.shape[1]
    outs, out_specs = column_outs(192, 1536, 256, 6)
    whole = pl.BlockSpec((768, tokens), lambda t: (0, 0))
    ycols = pl.BlockSpec((tokens, 256), lambda t: (0, jnp.where(t < 5, t, jnp.clip(t - 1, 4, 8))))
    dcols = pl.BlockSpec((tokens, 256), lambda t: (0, jnp.maximum(t - 9, 0)))
    return call(grad_qo_kernel, outs, [xo, xr, yo, yr, do, dr], 4e9, specs=[whole, whole, ycols, ycols, dcols, dcols],
                grid=(12,), out_specs=out_specs)


def grad_down_kernel(xo, xr, yo, yr, a_send, a_keep, b_send, b_keep):
    t = pl.program_id(0)
    acc = product_of_both(xo[...], xr[...], yo[...], yr[...])
    for k, out in enumerate((a_send, a_keep, b_send, b_keep)):
        @pl.when(t // 2 == k)
        def _():
            out[...] = acc


def grad_down(xo, xr, yo, yr):
    tokens, d_model = yo.shape

    def source(t):
        half = t // 4
        left = (t % 2) * 2 + 1 - (t // 2)
        right = (1 - (t // 2 - 2)) * 2 + t % 2
        return (jnp.where(half == 0, left, right) * 2 + half, 0)

    rows = pl.BlockSpec((192, tokens), source)
    whole = pl.BlockSpec((tokens, d_model), lambda t: (0, 0))
    out_specs = [pl.BlockSpec((192, d_model), (lambda k: lambda t: (jnp.clip(t - 2 * k, 0, 1), 0))(k)) for k in range(4)]
    return call(grad_down_kernel, [struct((384, d_model), F32)] * 4, [xo, xr, yo, yr], 4e9,
                specs=[rows, rows, whole, whole], grid=(8,), out_specs=out_specs)


def exchange_first(parts):
    a_send, a_keep, b_send, b_keep = parts
    return a_keep, permute(a_send, TO_X), b_keep, permute(b_send, TO_Y)


def exchange_second(parts, late):
    a_keep, a_got, b_keep, b_got = parts
    a_got, b_got = after(a_got, late), after(b_got, late)
    rows = a_keep.shape[0] // 2
    a_more = permute(a_keep[rows:] + a_got[rows:], TO_Y)
    b_more = permute(b_keep[rows:] + b_got[rows:], TO_X)
    return (a_keep[:rows], a_got[:rows], a_more), (b_keep[:rows], b_got[:rows], b_more)


def hold(parts, late):
    return tuple((p[0], p[1], after(p[2], late)) for p in parts)


def add_up(parts):
    return [(p[0] + p[1] + p[2]).astype(BF) for p in parts]


def finish(parts, axis):
    return jnp.concatenate(add_up(parts), axis=axis)


def small_pack_kernel(s0, q0, d0, u0, s1, q1, d1, u1, out):
    out[...] = jnp.zeros_like(out)
    for layer, (sums, qsum, dsum, usum) in enumerate(((s0, q0, d0, u0), (s1, q1, d1, u1))):
        base = layer * 8
        out[base:base + 2, 0:768] = sums[0:2, :]
        out[base + 2:base + 3, 0:2304] = regroup(qsum[...], 3, 2)
        out[base + 3:base + 4, 0:768] = dsum[...]
        out[base + 4:base + 6, 0:768] = sums[2:4, :]
        out[base + 6:base + 7, :] = usum[...]


def small_out_kernel(a_ref, b_ref, *outs):
    total = a_ref[...] + b_ref[...]
    node, xpos, core = my_place()
    dev = node * 4 + xpos * 2 + core
    for k, (out, width) in enumerate(zip(outs, (96, 96, 288, 96, 96, 96, 384))):
        for layer in range(2):
            row = total[layer * 8:layer * 8 + 8, :]
            turned = pltpu.roll(row, lax.rem(3072 - dev * width, 3072), 1)
            out[layer:layer + 1, :] = turned[k:k + 1, 0:width].astype(BF)


def small_sums(parts):
    total = call(small_pack_kernel, [struct((16, 3072), F32)], parts, 1e9)[0]
    total = total + permute(total, TO_C)
    total = total + permute(total, TO_X)
    more = permute(total, TO_Y)
    outs = [struct((2, w), BF) for w in (96, 96, 288, 96, 96, 96, 384)]
    return call(small_out_kernel, outs, [total, more], 1e9)


def rope_tables(seq):
    lane = jnp.arange(128)
    low = lane % 64 < 8
    high = (lane % 64 >= 8) & (lane % 64 < 16)
    inv_freq = 1.0 / (10000.0 ** (jnp.arange(0, 16, 2, dtype=F32) / 16))
    angles = jnp.arange(seq, dtype=F32)[:, None] * inv_freq[None, :]
    angles = jnp.tile(angles, (1, 16))
    return (jnp.where(low | high, jnp.cos(angles), 1.0), jnp.where(low, -jnp.sin(angles), 0.0),
            jnp.where(high, jnp.sin(angles), 0.0))


def after(value, *others):
    return lax.optimization_barrier((value,) + others)[0]


def device_step(x, y_cot, ln1_g, ln1_b, qkv_w, qkv_b, out_w, out_b, ln2_g, ln2_b, up_w, up_b, down_w, down_b):
    batch, seq, d_model = x.shape
    tokens = batch * seq
    h0 = x.reshape(tokens, d_model)
    cot = y_cot.reshape(tokens, d_model)
    smalls = jnp.concatenate([ln1_g, ln1_b, qkv_b, out_b, ln2_g, ln2_b, up_b, down_b], axis=1)
    extra = jnp.pad(smalls, ((0, 14), (0, 3072 - smalls.shape[1])))

    def qo_rows(i, weight):
        flat = weight[i].reshape(96, 6, 2, 3, 64).swapaxes(2, 3).reshape(96, 2304)
        return jnp.concatenate([flat, out_w[i]], axis=1)

    tables = rope_tables(seq)

    near_qo = gather_near(jnp.concatenate([qo_rows(0, qkv_w), extra], axis=0))
    near_up = gather_near(up_w[0])
    near_down = gather_near(down_w[0])
    rows1 = qo_rows(1, qkv_w)
    near_qo1 = gather_near(rows1)
    qo0, small = assemble_qo(gather_pieces(near_qo, 48))
    near_up1 = gather_near(up_w[1])
    near_down1 = gather_near(down_w[1])
    cot_rcv = permute(cot, TO_C)

    na0, nm0, qkv0, ctx0, res0 = attn_fwd(0, h0, qo0, small, tables)
    pieces_up = gather_pieces(near_up, 48, ctx0)
    pieces_down = gather_pieces(near_down, 192, ctx0)
    up0 = assemble(pieces_up)
    down0 = assemble(pieces_down)
    h1 = mlp_fwd(0, nm0, up0, down0, small, res0)
    qo1 = assemble(gather_pieces(near_qo1, 48, h1))
    na1, nm1, qkv1, ctx1, res1 = attn_fwd(1, h1, qo1, small, tables)

    def attn_back(d_out, w_qo, qkv, ctx, na, d_rcv):
        x_own, x_oth, dqkv, qsum, dsum = attn_bwd(d_out, w_qo, qkv, ctx, na, tables)
        x_rcv, y_rcv = permute(x_oth, TO_C), permute(dqkv, TO_C)
        dna = attn_in_bwd(dqkv, w_qo)
        parts = grad_qo(x_own, x_rcv, dqkv, y_rcv, d_out, d_rcv)
        return dna, qsum, dsum, parts

    dna1, qsum1, dsum1, parts = attn_back(cot, qo1, qkv1, ctx1, na1, cot_rcv)
    up1 = assemble(gather_pieces(near_up1, 48, dna1))
    down1 = assemble(gather_pieces(near_down1, 192, dna1))
    s_qo1 = exchange_first(parts)

    nm1 = after(nm1, parts[0])
    a_own, a_oth, m_own, m_oth, dpre, dnm1, usum1, y_out = mlp_bwd(1, nm1, cot, up1, down1, small, res1)
    a_rcv, m_rcv, p_rcv = permute(a_oth, TO_C), permute(m_oth, TO_C), permute(dpre, TO_C)
    d1, sums1 = norm_bwd(1, h1, cot, dna1, dnm1, small)
    d1_rcv = permute(d1, TO_C)
    parts = grad_down(a_own, after(a_rcv, d1), cot, cot_rcv)
    s_down1 = exchange_first(parts)
    parts = grad_up(m_own, after(m_rcv, parts[0]), dpre, p_rcv)
    s_up1 = exchange_first(parts)
    e_qo1 = exchange_second(s_qo1, dnm1)

    nm0 = after(nm0, parts[0])
    a_own, a_oth, m_own, m_oth, dpre, dnm0, usum0 = mlp_bwd(0, nm0, d1, up0, down0, small)
    a_rcv, m_rcv, p_rcv = permute(a_oth, TO_C), permute(m_oth, TO_C), permute(dpre, TO_C)
    e_down1 = exchange_second(s_down1, dnm0)
    parts = grad_down(a_own, a_rcv, d1, d1_rcv)
    s_down0 = exchange_first(parts)
    parts = grad_up(m_own, after(m_rcv, parts[0]), dpre, p_rcv)
    s_up0 = exchange_first(parts)

    d1_b = after(d1, parts[0])
    dna0, qsum0, dsum0, parts = attn_back(d1_b, qo0, qkv0, ctx0, na0, d1_rcv)
    s_qo0 = exchange_first(parts)
    x_grad, sums0 = norm_bwd(0, h0, d1, dna0, dnm0, small)
    g1, b1, gqb, gob, g2, b2, gub = small_sums([sums0, qsum0, dsum0, usum0, sums1, qsum1, dsum1, usum1])

    e_up1 = exchange_second(s_up1, s_up0[0])
    e_down0 = exchange_second(s_down0, dna0)
    e_up0 = exchange_second(s_up0, s_qo0[0])
    e_qo0 = exchange_second(s_qo0, s_qo0[0])
    e_qo1, e_down1, e_up1, e_down0 = (hold(e, s_qo0[0]) for e in (e_qo1, e_down1, e_up1, e_down0))

    def split_qo(parts):
        cols = add_up(parts)
        gqkv = jnp.concatenate([cols[0][:, 0:1280], cols[1][:, 0:1024]], axis=1)
        gout = jnp.concatenate([cols[0][:, 1280:], cols[1][:, 1024:]], axis=1)
        return gqkv.reshape(96, 6, 3, 2, 64).swapaxes(2, 3).reshape(96, 12, 192), gout

    gqkv0, gout0 = split_qo(e_qo0)
    gqkv1, gout1 = split_qo(e_qo1)
    gup = jnp.stack([finish(e_up0, 1), finish(e_up1, 1)])
    gdown = jnp.stack([finish(e_down0, 0), finish(e_down1, 0)])
    return (y_out.reshape(x.shape), x_grad.reshape(x.shape), g1, b1, jnp.stack([gqkv0, gqkv1]), gqb,
            jnp.stack([gout0, gout1]), gob, g2, b2, gup, gub, gdown, gob)


def solution(mesh):
    act_spec = P(AXES)
    param_spec = P(None, AXES)

    return jax.shard_map(device_step, mesh=mesh, in_specs=(act_spec, act_spec) + (param_spec,) * 12,
                         out_specs=(act_spec, act_spec) + (param_spec,) * 12, check_vma=False)
```

```python
import functools
import jax
import jax.numpy as jnp
from jax import lax
from jax.experimental import pallas as pl
from jax.experimental.pallas import tpu as pltpu
from jax.sharding import PartitionSpec as P

EPSILON = 1e-5
LIGHT = 1e9
HEAVY = 4e9
D_MODEL = 768
HIDDEN = 3072
SEQ = 128
SHARD = 96
PAIR = 384
TILE = 256
HEAD = 64
OCT = 8
PAD = 16
QKV = 2304
GCOLS = 1536
BLOCK = 192
WIDE = 512
BF = jnp.bfloat16
F32 = jnp.float32
AXES = ('node', 'local')
SQRT_HALF = 0.7071067811865476
INV_SQRT_2PI = 0.3989422804014327
VMEM = pl.BlockSpec(memory_space=pltpu.VMEM)
ANY = pl.BlockSpec(memory_space=pl.ANY)


def pairs(move):
    out = []
    for n in range(2):
        for x in range(2):
            for c in range(2):
                n2, x2, c2 = move(n, x, c)
                out.append((n * 4 + x * 2 + c, n2 * 4 + x2 * 2 + c2))
    return out


TO_X = pairs(lambda n, x, c: (n, 1 - x, c))
TO_Y = pairs(lambda n, x, c: (1 - n, x, c))
TO_C = pairs(lambda n, x, c: (n, x, 1 - c))


def permute(value, where):
    return lax.ppermute(value, AXES, where)


def my_place():
    node = lax.axis_index('node')
    local = lax.axis_index('local')
    return node, local // 2, local % 2


def dot_nn(a, b):
    return lax.dot_general(a, b, (((1,), (0,)), ((), ())), preferred_element_type=F32)


def dot_nt(a, b):
    return lax.dot_general(a, b, (((1,), (1,)), ((), ())), preferred_element_type=F32)


def dot_tn(a, b):
    return lax.dot_general(a, b, (((0,), (0,)), ((), ())), preferred_element_type=F32)


def call(kernel, outs, args, flops, scratch=(), specs=None, grid=(), out_specs=None, room=0):
    bytes_all = sum(a.size * a.dtype.itemsize for a in args) + sum(o.size * o.dtype.itemsize for o in outs)
    room = room or int(bytes_all / 2**20) + 14
    return pl.pallas_call(
        kernel, out_shape=outs, in_specs=specs or [VMEM] * len(args), out_specs=out_specs or [VMEM] * len(outs), grid=grid,
        scratch_shapes=list(scratch),
        cost_estimate=pl.CostEstimate(flops=int(flops), bytes_accessed=int(bytes_all), transcendentals=0),
        compiler_params=pltpu.CompilerParams(vmem_limit_bytes=room * 1024 * 1024))(*args)


def lane_mean(values):
    return jnp.mean(values, axis=-1, keepdims=True)


def row_sum(values):
    return jnp.sum(values, axis=0, keepdims=True)


def struct(shape, dtype):
    return jax.ShapeDtypeStruct(shape, dtype)


SMALL_WIDTHS = (SHARD, SHARD, 288, SHARD, SHARD, SHARD, PAIR, SHARD)


def gather_near(own):
    return own, permute(own, TO_X), permute(own, TO_Y)


def gather_pieces(near, half, late=None):
    own, from_x, from_y = near
    if late is not None:
        from_x, from_y = after(from_x, late), after(from_y, late)
    diag_a = permute(from_y[:half], TO_X)
    diag_b = permute(from_x[half:], TO_Y)
    mine = [own, from_x, from_y, diag_a, diag_b]
    return mine + [permute(piece, TO_C) for piece in mine]


def piece_places(rows):
    node, xpos, core = my_place()
    half = rows // 2
    out = []
    for side in range(2):
        cpos = core if side == 0 else 1 - core
        for k, (n, x, off, size) in enumerate(((node, xpos, 0, rows), (node, 1 - xpos, 0, rows), (1 - node, xpos, 0, rows),
                                               (1 - node, 1 - xpos, 0, half), (1 - node, 1 - xpos, half, half))):
            out.append((side * 5 + k, n * 4 + x * 2 + cpos, off, size))
    return out


def run_copies(copies):
    for copy in copies:
        copy.start()
    for copy in copies:
        copy.wait()


def regroup(line, outer, inner):
    starts = [base + (o * inner + i) * HEAD for base in range(0, QKV, PAIR) for i in range(inner) for o in range(outer)]
    return jnp.concatenate([line[:, t:t + HEAD] for t in starts], axis=1)


def assemble_qo_kernel(*refs):
    pieces, full, small_ref, raw, sems = refs[:10], refs[10], refs[11], refs[12], refs[13]
    copies = []
    for idx, dev, off, size in piece_places(SHARD):
        copies.append(pltpu.make_async_copy(
            pieces[idx].at[pl.ds(0, size), :], full.at[pl.ds(pl.multiple_of(dev * SHARD + off, PAD), size), :], sems.at[idx]))
        if off + size == SHARD:
            copies.append(pltpu.make_async_copy(
                pieces[idx].at[pl.ds(size, PAD), :], raw.at[pl.ds(pl.multiple_of(dev * PAD, PAD), PAD), :], sems.at[10 + idx]))
    run_copies(copies)
    for layer in range(2):
        rows = jnp.concatenate([raw[j * PAD:(j + 1) * PAD, :].astype(F32)[layer:layer + 1, :] for j in range(OCT)], axis=0)
        pos = 0
        for k, width in enumerate(SMALL_WIDTHS):
            line = jnp.concatenate([rows[j:j + 1, pos:pos + width] for j in range(OCT)], axis=1)
            if width == 288:
                line = regroup(line, 2, 3)
            small_ref[layer * OCT + k:layer * OCT + k + 1, 0:OCT * width] = line
            pos += width


def assemble_qo(pieces):
    return call(assemble_qo_kernel, [struct((D_MODEL, HIDDEN), BF), struct((PAD, HIDDEN), F32)], pieces, LIGHT,
            scratch=[pltpu.VMEM((SEQ, HIDDEN), BF), pltpu.SemaphoreType.DMA((20,))], specs=[ANY] * 10)


def assemble_kernel(*refs):
    pieces, full, sems = refs[:10], refs[10], refs[11]
    rows = full.shape[0] // OCT
    run_copies([pltpu.make_async_copy(
        pieces[idx], full.at[pl.ds(pl.multiple_of(dev * rows + off, PAD), size), :], sems.at[idx])
        for idx, dev, off, size in piece_places(rows)])


def assemble(pieces):
    rows, cols = pieces[0].shape
    return call(assemble_kernel, [struct((rows * OCT, cols), BF)], pieces, LIGHT,
                scratch=[pltpu.SemaphoreType.DMA((10,))], specs=[ANY] * 10)[0]


def rotate(block, cos_t, low_t, high_t):
    return block * cos_t + pltpu.roll(block, 120, 1) * low_t + pltpu.roll(block, OCT, 1) * high_t


def rotate_back(block, cos_t, low_t, high_t):
    return block * cos_t + pltpu.roll(block * low_t, OCT, 1) + pltpu.roll(block * high_t, 120, 1)


def softmax_down(scores):
    peak = jnp.max(scores, axis=0, keepdims=True)
    powers = jnp.exp(scores - peak)
    return powers * (1.0 / row_sum(powers))


def paired_mask(seq):
    keys = lax.broadcasted_iota(jnp.int32, (seq, seq), 0)
    queries = lax.broadcasted_iota(jnp.int32, (seq, seq), 1)
    return jnp.concatenate([queries >= keys] * 2, axis=1)


def by_head(block, left):
    zero = jnp.zeros_like(block)
    return jnp.concatenate([jnp.where(left, block, zero), jnp.where(left, zero, block)], axis=0)


def join_heads(stacked, left):
    rows = stacked.shape[0] // 2
    return jnp.where(left, stacked[:rows], stacked[rows:])


def attn_fwd_kernel(layer, h_ref, w_ref, small_ref, cos_ref, low_ref, high_ref,
                    na_ref, nm_ref, qkv_ref, ctx_ref, res_ref):
    tokens, d_model = h_ref.shape
    seq = cos_ref.shape[0]
    heads = d_model // HEAD

    def small(k, cols=slice(0, D_MODEL)):
        return small_ref[layer * OCT + k:layer * OCT + k + 1, cols]

    @pl.loop(0, tokens // seq)
    def _(s):
        rows = pl.ds(pl.multiple_of(s * seq, seq), seq)
        x = h_ref[rows, :].astype(F32)
        center = x - lane_mean(x)
        scaled = center * lax.rsqrt(lane_mean(center * center) + EPSILON)
        na_ref[rows, :] = (scaled * small(0) + small(1)).astype(BF)
        nm_ref[rows, :] = (scaled * small(4) + small(5)).astype(BF)

    @pl.loop(0, 3)
    def _(t):
        cols = pl.ds(pl.multiple_of(t * D_MODEL, D_MODEL), D_MODEL)
        val = dot_nn(na_ref[...], w_ref[:, cols]) + small(2, cols)
        for s in range(tokens // seq):
            rows = slice(s * seq, (s + 1) * seq)
            for part in range(6):
                piece = val[rows, part * SEQ:(part + 1) * SEQ]
                if part % 3 < 2:
                    piece = rotate(piece, cos_ref[...], low_ref[...], high_ref[...])
                qkv_ref[rows, pl.ds(pl.multiple_of(t * D_MODEL + part * SEQ, SEQ), SEQ)] = piece.astype(BF)

    mask = paired_mask(seq)
    left = lax.broadcasted_iota(jnp.int32, (seq, SEQ), 1) < HEAD

    @pl.loop(0, tokens // seq)
    def _(s):
        rows = pl.ds(pl.multiple_of(s * seq, seq), seq)
        for pair in range(heads // 2):
            base = pair * PAIR
            query = by_head(qkv_ref[rows, base:base + SEQ], left)
            key = qkv_ref[rows, base + SEQ:base + TILE]
            value = qkv_ref[rows, base + TILE:base + PAIR]
            scores = jnp.where(mask, dot_nt(key, query) * 0.125, -1e30)
            probs = softmax_down(scores).astype(BF)
            ctx_ref[rows, pair * SEQ:(pair + 1) * SEQ] = join_heads(dot_tn(probs, value), left).astype(BF)

    @pl.loop(0, 3)
    def _(t):
        cols = pl.ds(pl.multiple_of(t * TILE, TILE), TILE)
        wcols = pl.ds(pl.multiple_of(QKV + t * TILE, TILE), TILE)
        res_ref[:, cols] = (h_ref[:, cols].astype(F32)
                            + (dot_nn(ctx_ref[...], w_ref[:, wcols]) + small(3, cols)))


def attn_fwd(layer, h, w_qo, small, tables):
    tokens, d_model = h.shape
    outs = [struct((tokens, d_model), BF), struct((tokens, d_model), BF), struct((tokens, 3 * d_model), BF),
            struct((tokens, d_model), BF), struct((tokens, d_model), F32)]
    return call(functools.partial(attn_fwd_kernel, layer), outs, [h, w_qo, small, *tables], 20e9)


def split_rows(full_t, own_ref, other_ref, rows, base=0):
    node, xpos, core = my_place()
    for ry in range(2):
        for rx in range(2):
            n = node if ry == 0 else 1 - node
            x = xpos if rx == 0 else 1 - xpos
            for rc, out in ((0, own_ref), (1, other_ref)):
                c = core if rc == 0 else 1 - core
                start = pl.multiple_of((n * 4 + x * 2 + c) * rows, PAD)
                first = base + (ry * 2 + rx) * rows
                out[first:first + rows, :] = full_t[pl.ds(start, rows), :]


def transpose_to(src_ref, dst_ref):
    _, width = src_ref.shape

    @pl.loop(0, width // SEQ)
    def _(t):
        cols = pl.ds(pl.multiple_of(t * SEQ, SEQ), SEQ)
        dst_ref[cols, :] = src_ref[:, cols].T


def attn_bwd_kernel(d_ref, w_ref, qkv_ref, ctx_ref, na_ref, cos_ref, low_ref, high_ref,
                    x_own, x_oth, dqkv_ref, bsum_ref, dsum_ref, dctx_ref, turn_ref):
    tokens, d_model = d_ref.shape
    seq = cos_ref.shape[0]
    heads = d_model // HEAD

    @pl.loop(0, 3)
    def _(t):
        cols = pl.ds(pl.multiple_of(t * TILE, TILE), TILE)
        dctx_ref[:, cols] = dot_nt(d_ref[...], w_ref[cols, QKV:HIDDEN]).astype(BF)

    transpose_to(ctx_ref, turn_ref)
    split_rows(turn_ref, x_own, x_oth, d_model // OCT)
    transpose_to(na_ref, turn_ref)
    split_rows(turn_ref, x_own, x_oth, d_model // OCT, d_model // 2)

    bsum_ref[...] = jnp.zeros_like(bsum_ref)
    dsum_ref[...] = jnp.zeros_like(dsum_ref)
    mask = paired_mask(seq)
    left = lax.broadcasted_iota(jnp.int32, (seq, SEQ), 1) < HEAD

    @pl.loop(0, tokens // seq)
    def _(s):
        rows = pl.ds(pl.multiple_of(s * seq, seq), seq)
        dsum_ref[...] += row_sum(d_ref[rows, :].astype(F32))
        for pair in range(heads // 2):
            base = pair * PAIR
            query = by_head(qkv_ref[rows, base:base + SEQ], left)
            key = qkv_ref[rows, base + SEQ:base + TILE]
            value = qkv_ref[rows, base + TILE:base + PAIR]
            dctx = by_head(dctx_ref[rows, pair * SEQ:(pair + 1) * SEQ], left)
            scores = jnp.where(mask, dot_nt(key, query) * 0.125, -1e30)
            probs = softmax_down(scores)
            dprobs = dot_nt(value, dctx).astype(BF).astype(F32)
            dvalue = dot_nn(probs.astype(BF), dctx).astype(BF)
            dscores = (probs * (dprobs - row_sum(dprobs * probs)) * 0.125).astype(BF)
            dquery = join_heads(dot_tn(dscores, key), left).astype(BF)
            dkey = dot_nn(dscores, query).astype(BF)
            for part, piece in enumerate((dquery, dkey, dvalue)):
                turned = piece.astype(F32)
                if part < 2:
                    turned = rotate_back(turned, cos_ref[...], low_ref[...], high_ref[...])
                cols = slice(base + part * SEQ, base + part * SEQ + SEQ)
                bsum_ref[:, cols] += row_sum(turned)
                dqkv_ref[rows, cols] = turned.astype(BF)


def attn_bwd(d_out, w_qo, qkv, ctx, na, tables):
    tokens, d_model = d_out.shape
    outs = [struct((d_model, tokens), BF)] * 2 + [struct((tokens, 3 * d_model), BF),
                                                 struct((1, 3 * d_model), F32), struct((1, d_model), F32)]
    return call(attn_bwd_kernel, outs, [d_out, w_qo, qkv, ctx, na, *tables], 25e9,
                scratch=[pltpu.VMEM((tokens, d_model), BF), pltpu.VMEM((d_model, tokens), BF)])


def norm_in_kernel(dqkv_ref, w_ref, dna_ref):
    @pl.loop(0, 3)
    def _(t):
        cols = pl.ds(pl.multiple_of(t * TILE, TILE), TILE)
        dna_ref[:, cols] = dot_nt(dqkv_ref[...], w_ref[cols, 0:QKV]).astype(BF)


def attn_in_bwd(dqkv, w_qo):
    tokens, d_model = dqkv.shape[0], w_qo.shape[0]
    return call(norm_in_kernel, [struct((tokens, d_model), BF)], [dqkv, w_qo], 6e9)[0]


def mlp_fwd_kernel(layer, nm_ref, up_ref, down_ref, small_ref, res_ref, out_ref, act_ref):
    _, d_model = nm_ref.shape
    hidden = up_ref.shape[1]

    @pl.loop(0, hidden // WIDE)
    def _(t):
        cols = pl.ds(pl.multiple_of(t * WIDE, WIDE), WIDE)
        pre = dot_nn(nm_ref[...], up_ref[:, cols]) + small_ref[layer * OCT + 6:layer * OCT + 7, cols]
        act_ref[:, cols] = (0.5 * pre * (1.0 + lax.erf(pre * SQRT_HALF))).astype(BF)

    @pl.loop(0, d_model // TILE)
    def _(t):
        cols = pl.ds(pl.multiple_of(t * TILE, TILE), TILE)
        out_ref[:, cols] = (res_ref[:, cols] + (dot_nn(act_ref[...], down_ref[:, cols]) + small_ref[layer * OCT + 7:layer * OCT + OCT, cols])).astype(BF)


def mlp_fwd(layer, nm, w_up, w_down, small, res):
    tokens, d_model = nm.shape
    return call(functools.partial(mlp_fwd_kernel, layer), [struct((tokens, d_model), BF)], [nm, w_up, w_down, small, res],
                4 * tokens * d_model * w_up.shape[1], scratch=[pltpu.VMEM((tokens, w_up.shape[1]), BF)])[0]


def mlp_bwd_kernel(layer, with_out, *refs):
    nm_ref, d_ref, up_ref, down_ref, small_ref = refs[:5]
    refs = refs[5:]
    if with_out:
        res_ref = refs[0]
        refs = refs[1:]
    act_own, act_oth, nm_own, nm_oth, dpre_ref, dnm_ref, ubsum_ref = refs[:7]
    refs = refs[7:]
    if with_out:
        out_ref, sum_ref, turn_ref = refs
    else:
        turn_ref, = refs
    _, d_model = nm_ref.shape
    node, xpos, core = my_place()
    block = PAIR

    transpose_to(nm_ref, turn_ref)
    split_rows(turn_ref, nm_own, nm_oth, d_model // OCT)
    if with_out:
        sum_ref[...] = res_ref[...] + small_ref[layer * OCT + 7:layer * OCT + OCT, 0:D_MODEL]

    @pl.loop(0, 4)
    def _(t):
        n = (node + t // 2) % 2
        x = (xpos + t % 2) % 2
        cols = pl.ds(pl.multiple_of((n * 4 + x * 2) * block, 2 * block), 2 * block)
        pre = dot_nn(nm_ref[...], up_ref[:, cols]) + small_ref[layer * OCT + 6:layer * OCT + 7, cols]
        dact = dot_nt(d_ref[...], down_ref[cols, :]).astype(BF).astype(F32)
        cdf = 0.5 * (1.0 + lax.erf(pre * SQRT_HALF))
        act = (pre * cdf).astype(BF)
        dpre = dact * (cdf + pre * (jnp.exp(-0.5 * pre * pre) * INV_SQRT_2PI))
        ubsum_ref[0:1, cols] = row_sum(dpre)
        dpre_ref[:, cols] = dpre.astype(BF)
        place = pl.ds(pl.multiple_of(t * block, block), block)
        for c in range(2):
            @pl.when(core == c)
            def _():
                act_own[place, :] = act[:, c * block:(c + 1) * block].T

            @pl.when(core != c)
            def _():
                act_oth[place, :] = act[:, c * block:(c + 1) * block].T
        if with_out:
            sum_ref[...] += dot_nn(act, down_ref[cols, :])

    @pl.loop(0, d_model // TILE)
    def _(t):
        cols = pl.ds(pl.multiple_of(t * TILE, TILE), TILE)
        dnm_ref[:, cols] = dot_nt(dpre_ref[...], up_ref[cols, :]).astype(BF)

    if with_out:
        out_ref[...] = sum_ref[...].astype(BF)


def mlp_bwd(layer, nm, d_out, w_up, w_down, small, res=None):
    tokens, d_model = nm.shape
    hidden = w_up.shape[1]
    with_out = res is not None
    outs = [struct((hidden // 2, tokens), BF)] * 2 + [struct((d_model // 2, tokens), BF)] * 2
    outs += [struct((tokens, hidden), BF), struct((tokens, d_model), BF), struct((1, hidden), F32)]
    args = [nm, d_out, w_up, w_down, small]
    scratch = [pltpu.VMEM((d_model, tokens), BF)]
    if with_out:
        args += [res]
        outs += [struct((tokens, d_model), BF)]
        scratch = [pltpu.VMEM((tokens, d_model), F32)] + scratch
    return call(functools.partial(mlp_bwd_kernel, layer, with_out), outs, args,
                2 * tokens * d_model * hidden * (4 if with_out else 3), scratch=scratch)


def mlp_out_kernel(layer, own_ref, oth_ref, down_ref, small_ref, res_ref, out_ref, sum_ref):
    node, xpos, core = my_place()
    row = layer * OCT + 7
    sum_ref[...] = res_ref[...] + small_ref[row:row + 1, :D_MODEL]

    @pl.loop(0, 4)
    def _(t):
        n = (node + t // 2) % 2
        x = (xpos + t % 2) % 2
        place = pl.ds(pl.multiple_of(t * PAIR, PAIR), PAIR)
        for ref, c in ((own_ref, core), (oth_ref, 1 - core)):
            rows = pl.ds(pl.multiple_of((n * 4 + x * 2 + c) * PAIR, PAIR), PAIR)
            sum_ref[...] += dot_tn(ref[place, :], down_ref[rows, :])

    out_ref[...] = sum_ref[...].astype(BF)


def mlp_out(layer, act_own, act_oth, w_down, small, res):
    return call(functools.partial(mlp_out_kernel, layer), [struct(res.shape, BF)],
                [act_own, act_oth, w_down, small, res], HEAVY, scratch=[pltpu.VMEM(res.shape, F32)])[0]


def norm_bwd_kernel(layer, h_ref, d_ref, dna_ref, dnm_ref, small_ref, dh_ref, sums_ref):
    tokens, _ = h_ref.shape
    sums_ref[...] = jnp.zeros_like(sums_ref)

    @pl.loop(0, tokens // SEQ)
    def _(s):
        rows = pl.ds(pl.multiple_of(s * SEQ, SEQ), SEQ)
        x = h_ref[rows, :].astype(F32)
        center = x - lane_mean(x)
        inv = lax.rsqrt(lane_mean(center * center) + EPSILON)
        scaled = center * inv
        da = dna_ref[rows, :].astype(F32)
        dm = dnm_ref[rows, :].astype(F32)
        sums_ref[0:1, :] += row_sum(da * scaled)
        sums_ref[1:2, :] += row_sum(da)
        sums_ref[2:3, :] += row_sum(dm * scaled)
        sums_ref[3:4, :] += row_sum(dm)
        dscaled = da * small_ref[layer * OCT:layer * OCT + 1, 0:D_MODEL] + dm * small_ref[layer * OCT + 4:layer * OCT + 5, 0:D_MODEL]
        dh = inv * (dscaled - lane_mean(dscaled)
                    - scaled * lane_mean(dscaled * scaled))
        dh_ref[rows, :] = (d_ref[rows, :].astype(F32) + dh).astype(BF)


def norm_bwd(layer, h, d_out, dna, dnm, small):
    tokens, d_model = h.shape
    return call(functools.partial(norm_bwd_kernel, layer), [struct((tokens, d_model), BF), struct((OCT, d_model), F32)],
                [h, d_out, dna, dnm, small], HEAVY)


def product_of_both(xo, xr, yo, yr):
    return dot_nn(xo, yo) + dot_nn(xr, yr)


def put_columns(acc, t, half_tiles, a_send, a_keep, b_send, b_keep):
    rows = acc.shape[0] // 4

    @pl.when(t < half_tiles)
    def _():
        for k, (out, pos) in enumerate(((a_keep, 0), (a_send, 0), (a_keep, 1), (a_send, 1))):
            out[pos * rows:(pos + 1) * rows, :] = acc[k * rows:(k + 1) * rows, :]

    @pl.when(t >= half_tiles)
    def _():
        for k, (out, pos) in enumerate(((b_keep, 0), (b_keep, 1), (b_send, 0), (b_send, 1))):
            out[pos * rows:(pos + 1) * rows, :] = acc[k * rows:(k + 1) * rows, :]


def column_outs(rows, cols, tile, half_tiles):
    left = pl.BlockSpec((rows, tile), lambda t: (0, jnp.minimum(t, half_tiles - 1)))
    right = pl.BlockSpec((rows, tile), lambda t: (0, jnp.maximum(t - half_tiles, 0)))
    return [struct((rows, cols), F32)] * 4, [left, left, right, right]


def grad_up_kernel(xo, xr, yo, yr, *outs):
    put_columns(product_of_both(xo[...], xr[...], yo[...], yr[...]), pl.program_id(0), 3, *outs)


def grad_up(xo, xr, yo, yr):
    tokens = xo.shape[1]
    outs, out_specs = column_outs(BLOCK, GCOLS, WIDE, 3)
    whole = pl.BlockSpec((PAIR, tokens), lambda t: (0, 0))
    cols = pl.BlockSpec((tokens, WIDE), lambda t: (0, t))
    return call(grad_up_kernel, outs, [xo, xr, yo, yr], HEAVY, specs=[whole, whole, cols, cols], grid=(6,),
                out_specs=out_specs)


def grad_qo_kernel(xo, xr, yo, yr, do, dr, *outs):
    t = pl.program_id(0)
    from_out = (t == 5) | (t >= 10)

    @pl.when(from_out)
    def _():
        put_columns(product_of_both(xo[0:PAIR, :], xr[0:PAIR, :], do[...], dr[...]), t, 6, *outs)

    @pl.when(jnp.logical_not(from_out))
    def _():
        put_columns(product_of_both(xo[PAIR:D_MODEL, :], xr[PAIR:D_MODEL, :], yo[...], yr[...]), t, 6, *outs)


def grad_qo(xo, xr, yo, yr, do, dr):
    tokens = xo.shape[1]
    outs, out_specs = column_outs(BLOCK, GCOLS, TILE, 6)
    whole = pl.BlockSpec((D_MODEL, tokens), lambda t: (0, 0))
    ycols = pl.BlockSpec((tokens, TILE), lambda t: (0, jnp.where(t < 5, t, jnp.clip(t - 1, 4, OCT))))
    dcols = pl.BlockSpec((tokens, TILE), lambda t: (0, jnp.maximum(t - 9, 0)))
    return call(grad_qo_kernel, outs, [xo, xr, yo, yr, do, dr], HEAVY, specs=[whole, whole, ycols, ycols, dcols, dcols],
                grid=(12,), out_specs=out_specs)


def grad_down_kernel(xo, xr, yo, yr, a_send, a_keep, b_send, b_keep):
    t = pl.program_id(0)
    acc = product_of_both(xo[...], xr[...], yo[...], yr[...])
    for k, out in enumerate((a_send, a_keep, b_send, b_keep)):
        @pl.when(t // 2 == k)
        def _():
            out[...] = acc


def grad_down(xo, xr, yo, yr):
    tokens, d_model = yo.shape

    def source(t):
        half = t // 4
        left = (t % 2) * 2 + 1 - (t // 2)
        right = (1 - (t // 2 - 2)) * 2 + t % 2
        return (jnp.where(half == 0, left, right) * 2 + half, 0)

    rows = pl.BlockSpec((BLOCK, tokens), source)
    whole = pl.BlockSpec((tokens, d_model), lambda t: (0, 0))
    out_specs = [pl.BlockSpec((BLOCK, d_model), (lambda k: lambda t: (jnp.clip(t - 2 * k, 0, 1), 0))(k)) for k in range(4)]
    return call(grad_down_kernel, [struct((PAIR, d_model), F32)] * 4, [xo, xr, yo, yr], HEAVY,
                specs=[rows, rows, whole, whole], grid=(OCT,), out_specs=out_specs)


def exchange_first(parts):
    a_send, a_keep, b_send, b_keep = parts
    return a_keep, permute(a_send, TO_X), b_keep, permute(b_send, TO_Y)


def exchange_second(parts, late):
    a_keep, a_got, b_keep, b_got = parts
    a_got, b_got = after(a_got, late), after(b_got, late)
    rows = a_keep.shape[0] // 2
    a_more = permute(a_keep[rows:] + a_got[rows:], TO_Y)
    b_more = permute(b_keep[rows:] + b_got[rows:], TO_X)
    return (a_keep[:rows], a_got[:rows], a_more), (b_keep[:rows], b_got[:rows], b_more)


def hold(parts, late):
    return tuple((p[0], p[1], after(p[2], late)) for p in parts)


def add_up(parts):
    return [(p[0] + p[1] + p[2]).astype(BF) for p in parts]


def finish(parts, axis):
    return jnp.concatenate(add_up(parts), axis=axis)


def small_pack_kernel(s0, q0, d0, u0, s1, q1, d1, u1, out):
    out[...] = jnp.zeros_like(out)
    for layer, (sums, qsum, dsum, usum) in enumerate(((s0, q0, d0, u0), (s1, q1, d1, u1))):
        base = layer * OCT
        out[base:base + 2, 0:D_MODEL] = sums[0:2, :]
        out[base + 2:base + 3, 0:QKV] = regroup(qsum[...], 3, 2)
        out[base + 3:base + 4, 0:D_MODEL] = dsum[...]
        out[base + 4:base + 6, 0:D_MODEL] = sums[2:4, :]
        out[base + 6:base + 7, :] = usum[...]


def small_out_kernel(a_ref, b_ref, *outs):
    total = a_ref[...] + b_ref[...]
    node, xpos, core = my_place()
    dev = node * 4 + xpos * 2 + core
    for k, (out, width) in enumerate(zip(outs, (SHARD, SHARD, 288, SHARD, SHARD, SHARD, PAIR))):
        for layer in range(2):
            row = total[layer * OCT:layer * OCT + OCT, :]
            turned = pltpu.roll(row, lax.rem(HIDDEN - dev * width, HIDDEN), 1)
            out[layer:layer + 1, :] = turned[k:k + 1, 0:width].astype(BF)


def small_sums(parts):
    total = call(small_pack_kernel, [struct((PAD, HIDDEN), F32)], parts, LIGHT)[0]
    total = total + permute(total, TO_C)
    total = total + permute(total, TO_X)
    more = permute(total, TO_Y)
    outs = [struct((2, w), BF) for w in (SHARD, SHARD, 288, SHARD, SHARD, SHARD, PAIR)]
    return call(small_out_kernel, outs, [total, more], LIGHT)


def rope_tables(seq):
    lane = jnp.arange(SEQ)
    low = lane % HEAD < OCT
    high = (lane % HEAD >= OCT) & (lane % HEAD < PAD)
    inv_freq = 1.0 / (10000.0 ** (jnp.arange(0, PAD, 2, dtype=F32) / PAD))
    angles = jnp.arange(seq, dtype=F32)[:, None] * inv_freq[None, :]
    angles = jnp.tile(angles, (1, PAD))
    return (jnp.where(low | high, jnp.cos(angles), 1.0), jnp.where(low, -jnp.sin(angles), 0.0),
            jnp.where(high, jnp.sin(angles), 0.0))


def after(value, *others):
    return lax.optimization_barrier((value,) + others)[0]


def device_step(x, y_cot, ln1_g, ln1_b, qkv_w, qkv_b, out_w, out_b, ln2_g, ln2_b, up_w, up_b, down_w, down_b):
    batch, seq, d_model = x.shape
    tokens = batch * seq
    h0 = x.reshape(tokens, d_model)
    cot = y_cot.reshape(tokens, d_model)
    smalls = jnp.concatenate([ln1_g, ln1_b, qkv_b, out_b, ln2_g, ln2_b, up_b, down_b], axis=1)
    extra = jnp.pad(smalls, ((0, 14), (0, HIDDEN - smalls.shape[1])))

    def qo_rows(i, weight):
        flat = weight[i].reshape(SHARD, 6, 2, 3, HEAD).swapaxes(2, 3).reshape(SHARD, QKV)
        return jnp.concatenate([flat, out_w[i]], axis=1)

    tables = rope_tables(seq)

    near_qo = gather_near(jnp.concatenate([qo_rows(0, qkv_w), extra], axis=0))
    near_up = gather_near(up_w[0])
    near_down = gather_near(down_w[0])
    rows1 = qo_rows(1, qkv_w)
    near_qo1 = gather_near(rows1)
    qo0, small = assemble_qo(gather_pieces(near_qo, 48))
    near_up1 = gather_near(up_w[1])
    near_down1 = gather_near(down_w[1])
    cot_rcv = permute(cot, TO_C)

    na0, nm0, qkv0, ctx0, res0 = attn_fwd(0, h0, qo0, small, tables)
    pieces_up = gather_pieces(near_up, 48, ctx0)
    pieces_down = gather_pieces(near_down, BLOCK, ctx0)
    up0 = assemble(pieces_up)
    down0 = assemble(pieces_down)
    h1 = mlp_fwd(0, nm0, up0, down0, small, res0)
    qo1 = assemble(gather_pieces(near_qo1, 48, h1))
    na1, nm1, qkv1, ctx1, res1 = attn_fwd(1, h1, qo1, small, tables)

    def attn_back(d_out, w_qo, qkv, ctx, na, d_rcv):
        x_own, x_oth, dqkv, qsum, dsum = attn_bwd(d_out, w_qo, qkv, ctx, na, tables)
        x_rcv, y_rcv = permute(x_oth, TO_C), permute(dqkv, TO_C)
        dna = attn_in_bwd(dqkv, w_qo)
        parts = grad_qo(x_own, x_rcv, dqkv, y_rcv, d_out, d_rcv)
        return dna, qsum, dsum, parts

    dna1, qsum1, dsum1, parts = attn_back(cot, qo1, qkv1, ctx1, na1, cot_rcv)
    up1 = assemble(gather_pieces(near_up1, 48, dna1))
    down1 = assemble(gather_pieces(near_down1, BLOCK, dna1))
    s_qo1 = exchange_first(parts)

    nm1 = after(nm1, parts[0])
    a_own, a_oth, m_own, m_oth, dpre, dnm1, usum1 = mlp_bwd(1, nm1, cot, up1, down1, small)
    act1 = (a_own, a_oth)
    a_rcv, m_rcv, p_rcv = permute(a_oth, TO_C), permute(m_oth, TO_C), permute(dpre, TO_C)
    d1, sums1 = norm_bwd(1, h1, cot, dna1, dnm1, small)
    d1_rcv = permute(d1, TO_C)
    parts = grad_down(a_own, after(a_rcv, d1), cot, cot_rcv)
    s_down1 = exchange_first(parts)
    parts = grad_up(m_own, after(m_rcv, parts[0]), dpre, p_rcv)
    s_up1 = exchange_first(parts)
    e_qo1 = exchange_second(s_qo1, dnm1)

    nm0 = after(nm0, parts[0])
    a_own, a_oth, m_own, m_oth, dpre, dnm0, usum0 = mlp_bwd(0, nm0, d1, up0, down0, small)
    a_rcv, m_rcv, p_rcv = permute(a_oth, TO_C), permute(m_oth, TO_C), permute(dpre, TO_C)
    e_down1 = exchange_second(s_down1, dnm0)
    parts = grad_down(a_own, a_rcv, d1, d1_rcv)
    s_down0 = exchange_first(parts)
    parts = grad_up(m_own, after(m_rcv, parts[0]), dpre, p_rcv)
    s_up0 = exchange_first(parts)

    d1_b = after(d1, parts[0])
    dna0, qsum0, dsum0, parts = attn_back(d1_b, qo0, qkv0, ctx0, na0, d1_rcv)
    s_qo0 = exchange_first(parts)
    x_grad, sums0 = norm_bwd(0, h0, d1, dna0, dnm0, small)
    g1, b1, gqb, gob, g2, b2, gub = small_sums([sums0, qsum0, dsum0, usum0, sums1, qsum1, dsum1, usum1])

    e_up1 = exchange_second(s_up1, s_up0[0])
    e_down0 = exchange_second(s_down0, dna0)
    e_up0 = exchange_second(s_up0, s_qo0[0])
    y_out = mlp_out(1, after(act1[0], s_qo0[0]), act1[1], down1, small, res1)
    e_qo0 = exchange_second(s_qo0, s_qo0[0])
    e_qo1, e_down1, e_up1, e_down0 = (hold(e, s_qo0[0]) for e in (e_qo1, e_down1, e_up1, e_down0))

    def split_qo(parts):
        cols = add_up(parts)
        gqkv = jnp.concatenate([cols[0][:, 0:1280], cols[1][:, 0:1024]], axis=1)
        gout = jnp.concatenate([cols[0][:, 1280:], cols[1][:, 1024:]], axis=1)
        return gqkv.reshape(SHARD, 6, 3, 2, HEAD).swapaxes(2, 3).reshape(SHARD, 12, BLOCK), gout

    gqkv0, gout0 = split_qo(e_qo0)
    gqkv1, gout1 = split_qo(e_qo1)
    gup = jnp.stack([finish(e_up0, 1), finish(e_up1, 1)])
    gdown = jnp.stack([finish(e_down0, 0), finish(e_down1, 0)])
    return (y_out.reshape(x.shape), x_grad.reshape(x.shape), g1, b1, jnp.stack([gqkv0, gqkv1]), gqb,
            jnp.stack([gout0, gout1]), gob, g2, b2, gup, gub, gdown, gob)


def solution(mesh):
    act_spec = P(AXES)
    param_spec = P(None, AXES)

    return jax.shard_map(device_step, mesh=mesh, in_specs=(act_spec, act_spec) + (param_spec,) * 12,
                         out_specs=(act_spec, act_spec) + (param_spec,) * 12, check_vma=False)
```
